128 devices in a mesh: patch: 32 (over y, z, core), hidden: 4 (over x).
Axes of the slice: x: 4, y: 4, z: 4, core: 2. Of those that a mesh axis runs over, the one named last changes fastest.
Arguments:
- nodes: bfloat16 [65536, 512], P('patch', 'hidden'), may hold values from -6 to 6
- edges: bfloat16 [262144, 512], P(('patch', 'hidden')), may hold values from -6 to 6
- senders: int32 [262144], P(('patch', 'hidden')), may hold values from 0 to 4351
- receivers: int32 [262144], P(('patch', 'hidden')), may hold values from 0 to 2047
- halo_rows: int32 [32, 2, 1024], P('patch'), may hold values from 0 to 2047
- coarse_rows: int32 [32, 32, 8], P('patch'), may hold values from 0 to 63
- edge_count: int32 [128], P(('patch', 'hidden')), may hold values from 1024 to 2048, as said below
- w_edge_in: bfloat16 [1536, 512], replicated, may hold values from -0.15625 to 0.15625
- b_edge_in: float32 [512], replicated, may hold values from -3 to 3
- w_edge_out: bfloat16 [512, 512], replicated, may hold values from -0.25 to 0.25
- b_edge_out: float32 [512], replicated, may hold values from -2 to 2
- edge_gain: float32 [512], replicated, may hold values from 0.5 to 1.5
- edge_shift: float32 [512], replicated, may hold values from -1 to 1
- w_node_in: bfloat16 [1024, 512], replicated, may hold values from -0.1875 to 0.1875
- b_node_in: float32 [512], replicated, may hold values from -3 to 3
- w_node_out: bfloat16 [512, 512], replicated, may hold values from -0.25 to 0.25
- b_node_out: float32 [512], replicated, may hold values from -2 to 2
- node_gain: float32 [512], replicated, may hold values from 0.5 to 1.5
- node_shift: float32 [512], replicated, may hold values from -1 to 1
Outputs:
- nodes_out: bfloat16 [65536, 512], P('patch', 'hidden')
- edges_out: bfloat16 [262144, 512], P(('patch', 'hidden'))
The draws below stay inside these ranges and needn't reach their ends.
Inputs may be any that keep to these rules, and one draw needn't show every extreme that they name: `edge_count`: some block holds 2048 live edges.
All inputs are finite; a program needn't handle non-finite values.
Results may differ from the reference program's by a relative error of at most 0.007.
Values may be sent and summed in bfloat16 or wider, within the bound.
A program may use at most 128 MiB of HBM per device.

```python
import jax
import jax.numpy as jnp
from jax import lax

D = 512
NODE_DEV = 2048
EDGE_DEV = 2048
COARSE_DEV = 64
SLOT = 8
HALO = 1024
PATCHES = 32
SHARDS = 128
NODES = 65536
EDGES = 262144
TABLE = 4352
N_HIDDEN = 4


def draw_edge_count(key, part):
    draw_key, pick_key = jax.random.split(jax.random.fold_in(key, 11))
    counts = jax.random.randint(draw_key, (SHARDS,), EDGE_DEV // 2, EDGE_DEV + 1)
    busiest = jax.random.randint(pick_key, (), 0, SHARDS)
    return jnp.where(jnp.arange(SHARDS) == busiest, EDGE_DEV, counts).astype(jnp.int32)


def with_ends(result, rng, least, high):
    longest = result.shape.index(max(result.shape))
    spots = []
    for shift in (0, 1):
        where = [jax.random.randint(jax.random.fold_in(rng, axis), (), 0, length) for axis, length in enumerate(result.shape)]
        where[longest] = (where[longest] + shift) % result.shape[longest]
        spots.append(tuple(where))
    return result.at[spots[0]].set(least).at[spots[1]].set(high)


def shard_levels(own_key, dims, shards, least, high):
    def one(dim, parts):
        steps = jax.random.uniform(jax.random.fold_in(jax.random.fold_in(own_key, 6), dim), (parts,), jnp.float32, least / len(shards), high / len(shards))
        return jnp.repeat(jnp.exp(steps), dims[dim] // parts).reshape((-1,) + (1,) * (len(dims) - dim - 1))

    loudness = one(*shards[0])
    for cut in shards[1:]:
        loudness = loudness * one(*cut)
    return loudness


def gaussian(own_key, shape, deviation, most, pieces=(), kind=jnp.bfloat16):
    result = deviation * jax.random.normal(own_key, shape, jnp.float32)
    if pieces:
        result = result * shard_levels(own_key, shape, pieces, -0.22, 0.18)
    return jnp.clip(result, -most, most).astype(kind)


def setup_inputs(seed: int = 0) -> dict:
    seeds = jax.random.split(jax.random.key(seed), 20)
    nodes = gaussian(seeds[0], (NODES, D), 1.0, 6.0, ((0, 32), (1, 4)))
    edges = gaussian(seeds[1], (EDGES, D), 1.0, 6.0, ((0, 128),))
    senders = with_ends(jax.random.randint(seeds[2], (EDGES,), 0, TABLE), jax.random.fold_in(seeds[2], 1), 0, TABLE - 1).astype(jnp.int32)
    receivers = with_ends(jax.random.randint(seeds[3], (EDGES,), 0, NODE_DEV), jax.random.fold_in(seeds[3], 1), 0, NODE_DEV - 1).astype(jnp.int32)
    halo_rows = with_ends(jax.random.randint(seeds[4], (PATCHES, 2, HALO), 0, NODE_DEV), jax.random.fold_in(seeds[4], 1), 0, NODE_DEV - 1).astype(jnp.int32)
    coarse_rows = with_ends(jax.random.randint(seeds[5], (PATCHES, PATCHES, SLOT), 0, COARSE_DEV), jax.random.fold_in(seeds[5], 1), 0, COARSE_DEV - 1).astype(jnp.int32)
    edge_count = draw_edge_count(jax.random.fold_in(seeds[19], 71), 0)
    w_edge_in = gaussian(seeds[7], (3 * D, D), (3 * D) ** -0.5, 0.15625)
    b_edge_in = gaussian(seeds[8], (D,), 0.5, 3.0, (), jnp.float32)
    w_edge_out = gaussian(seeds[9], (D, D), D ** -0.5, 0.25)
    b_edge_out = gaussian(seeds[10], (D,), 0.3, 2.0, (), jnp.float32)
    edge_gain = jnp.clip(1.0 + 0.1 * jax.random.normal(seeds[11], (D,), jnp.float32), 0.5, 1.5)
    edge_shift = gaussian(seeds[12], (D,), 0.2, 1.0, (), jnp.float32)
    w_node_in = gaussian(seeds[13], (2 * D, D), (2 * D) ** -0.5, 0.1875)
    b_node_in = gaussian(seeds[14], (D,), 0.5, 3.0, (), jnp.float32)
    w_node_out = gaussian(seeds[15], (D, D), D ** -0.5, 0.25)
    b_node_out = gaussian(seeds[16], (D,), 0.3, 2.0, (), jnp.float32)
    node_gain = jnp.clip(1.0 + 0.1 * jax.random.normal(seeds[17], (D,), jnp.float32), 0.5, 1.5)
    node_shift = gaussian(seeds[18], (D,), 0.2, 1.0, (), jnp.float32)
    return {"nodes": nodes, "edges": edges, "senders": senders, "receivers": receivers, "halo_rows": halo_rows, "coarse_rows": coarse_rows, "edge_count": edge_count, "w_edge_in": w_edge_in, "b_edge_in": b_edge_in, "w_edge_out": w_edge_out, "b_edge_out": b_edge_out, "edge_gain": edge_gain, "edge_shift": edge_shift, "w_node_in": w_node_in, "b_node_in": b_node_in, "w_node_out": w_node_out, "b_node_out": b_node_out, "node_gain": node_gain, "node_shift": node_shift}


layer_epsilon = 1e-05

def perceptron(inputs, weight_in, bias_in, weight_out, bias_out, norm_gain, norm_shift):
    joined = jnp.concatenate(inputs, axis=1)
    hidden = jnp.dot(joined, weight_in, preferred_element_type=jnp.float32) + bias_in
    active = jax.nn.silu(hidden).astype(jnp.bfloat16)
    output = jnp.dot(active, weight_out, preferred_element_type=jnp.float32) + bias_out
    row_mean = lax.optimization_barrier(jnp.mean(output, axis=1, keepdims=True))
    row_var = lax.optimization_barrier(jnp.mean(jnp.square(output - row_mean), axis=1, keepdims=True))
    return (output - row_mean) * lax.rsqrt(row_var + layer_epsilon) * norm_gain + norm_shift

def block_segments(values, targets):
    return jax.ops.segment_sum(values, targets, num_segments=NODE_DEV)

def reference(nodes, edges, senders, receivers, halo_rows, coarse_rows, edge_count, w_edge_in, b_edge_in, w_edge_out, b_edge_out, edge_gain, edge_shift, w_node_in, b_node_in, w_node_out, b_node_out, node_gain, node_shift):
    patch_edges = N_HIDDEN * EDGE_DEV

    def patch_work(patch_id):
        first_edge = patch_id * patch_edges
        latent = lax.dynamic_slice_in_dim(edges, first_edge, patch_edges, 0)
        sender_code = lax.dynamic_slice_in_dim(senders, first_edge, patch_edges, 0)
        target = lax.dynamic_slice_in_dim(receivers, first_edge, patch_edges, 0)
        counts = lax.dynamic_slice_in_dim(edge_count, patch_id * N_HIDDEN, N_HIDDEN, 0)
        previous = jnp.mod(patch_id - 1, PATCHES).astype(jnp.int32)
        following = jnp.mod(patch_id + 1, PATCHES).astype(jnp.int32)
        from_previous = halo_rows[previous, 1][jnp.clip(sender_code - NODE_DEV, 0, HALO - 1)]
        from_following = halo_rows[following, 0][jnp.clip(sender_code - NODE_DEV - HALO, 0, HALO - 1)]
        far_slot = jnp.clip(sender_code - NODE_DEV - 2 * HALO, 0, PATCHES * SLOT - 1)
        far_owner = far_slot // SLOT
        far_row = coarse_rows[patch_id][far_owner, far_slot % SLOT]
        source = jnp.where(sender_code < NODE_DEV, patch_id * NODE_DEV + sender_code, jnp.where(sender_code < NODE_DEV + HALO, previous * NODE_DEV + from_previous, jnp.where(sender_code < NODE_DEV + 2 * HALO, following * NODE_DEV + from_following, far_owner * NODE_DEV + far_row))).astype(jnp.int32)
        sender_rows = nodes[source]
        patch_nodes = lax.dynamic_slice_in_dim(nodes, patch_id * NODE_DEV, NODE_DEV, 0)
        receiver_rows = patch_nodes[target]
        update = perceptron((latent, sender_rows, receiver_rows), w_edge_in, b_edge_in, w_edge_out, b_edge_out, edge_gain, edge_shift)
        position = jnp.arange(patch_edges, dtype=jnp.int32)
        live_mask = position % EDGE_DEV < counts[position // EDGE_DEV]
        message = jnp.where(live_mask[:, None], update, jnp.zeros_like(update))
        new_latent = (latent.astype(jnp.float32) + message).astype(jnp.bfloat16)
        sent = lax.optimization_barrier(message.astype(jnp.bfloat16)).astype(jnp.float32)
        partial_sums = jax.vmap(block_segments)(sent.reshape(N_HIDDEN, EDGE_DEV, D), target.reshape(N_HIDDEN, EDGE_DEV))
        rounded = lax.optimization_barrier(partial_sums.astype(jnp.bfloat16)).astype(jnp.float32)
        node_sums = lax.optimization_barrier(jnp.sum(rounded, axis=0))
        return (new_latent, node_sums)
    new_edges, node_sums = lax.map(patch_work, jnp.arange(PATCHES, dtype=jnp.int32))
    edges_out = new_edges.reshape(EDGES, D)
    gathered = node_sums.reshape(NODES, D).astype(jnp.bfloat16)
    update = perceptron((nodes, gathered), w_node_in, b_node_in, w_node_out, b_node_out, node_gain, node_shift)
    nodes_out = (nodes.astype(jnp.float32) + update).astype(jnp.bfloat16)
    return (nodes_out, edges_out)
```

```python
import jax
import jax.numpy as jnp
from jax import lax
from jax.experimental import pallas as pl
from jax.experimental.pallas import tpu as pltpu
from jax.sharding import PartitionSpec as P

COARSE_DEV = 64
LANES = 128
EDGE_BLOCK = 512


layer_epsilon = 1e-05


def in_order(blocks, dim):
    lengths = list(blocks.shape[1:])
    lengths[dim] *= blocks.shape[0]
    return jnp.moveaxis(blocks, 0, dim).reshape(lengths)


def from_everyone(array, axis):
    count = lax.axis_size(axis)
    return lax.all_to_all(
        jnp.broadcast_to(array[None], (count, *array.shape)), axis, 0, 0, tiled=True
    )


def collect(array, axis, dim):
    return in_order(from_everyone(array, axis), dim)


def extended(block, sides, width):
    for axis, dim in sides:
        count = lax.axis_size(axis)
        forward = [(i, i + 1) for i in range(count - 1)]
        forward.append((count - 1, 0))
        backward = [(target, source) for source, target in forward]
        low = lax.ppermute(
            lax.slice_in_dim(block, block.shape[dim] - width, None, axis=dim), axis, forward
        )
        high = lax.ppermute(lax.slice_in_dim(block, 0, width, axis=dim), axis, backward)
        block = jnp.concatenate([low, block, high], axis=dim)
    return block


def in_blocks(array, dim, count):
    lengths = array.shape
    blocks = array.reshape(*lengths[:dim], count, lengths[dim] // count, *lengths[dim + 1 :])
    return jnp.moveaxis(blocks, dim, 0)


def sent_and_summed(array, axis, dim):
    blocks = in_blocks(array, dim, lax.axis_size(axis))
    arrived = lax.all_to_all(blocks, axis, split_axis=0, concat_axis=0, tiled=True)
    return arrived.astype(jnp.float32).sum(axis=0)


def normalize(output, norm_gain, norm_shift):
    row_mean = jnp.mean(output, axis=1, keepdims=True)
    centered = output - row_mean
    row_var = jnp.mean(jnp.square(centered), axis=1, keepdims=True)
    return centered * lax.rsqrt(row_var + layer_epsilon) * norm_gain + norm_shift


def silu(v):
    half = 0.5 * v
    return half + half * jnp.tanh(half)


def column_of(ids_ref, row):
    return jnp.broadcast_to(ids_ref[pl.ds(row, 1), :], (LANES, LANES)).T


def one_hot_rows(ids_ref, first_row, rows, out_ref):
    width = out_ref.shape[1]
    lane = lax.broadcasted_iota(jnp.int32, (LANES, LANES), 1)
    for r in range(rows):
        ids = column_of(ids_ref, first_row + r)
        for k in range(width // LANES):
            out_ref[r * LANES : (r + 1) * LANES, k * LANES : (k + 1) * LANES] = jnp.where(
                ids == lane + k * LANES, 1.0, 0.0
            ).astype(jnp.bfloat16)


def edge_kernel(
    count_ref,
    table_ref,
    edges_ref,
    senders_ref,
    receivers_ref,
    w_in_ref,
    b_in_ref,
    w_out_ref,
    b_out_ref,
    gain_ref,
    shift_ref,
    edges_out_ref,
    sums_ref,
    hot_send,
    hot_recv,
    hot_sum,
    joined,
    sent,
):
    rows, columns = edges_ref.shape
    node_rows = sums_ref.shape[0]
    per = EDGE_BLOCK // LANES

    def edge_block(i, carry):
        start = pl.multiple_of(i * EDGE_BLOCK, EDGE_BLOCK)
        here = pl.ds(start, EDGE_BLOCK)
        one_hot_rows(senders_ref, i * per, per, hot_send)
        one_hot_rows(receivers_ref, i * per, per, hot_recv)
        latent = edges_ref[here, :]
        joined[:, :columns] = latent
        joined[:, columns : 2 * columns] = jnp.dot(
            hot_send[...], table_ref[...], preferred_element_type=jnp.float32
        ).astype(jnp.bfloat16)
        joined[:, 2 * columns :] = jnp.dot(
            hot_recv[...], table_ref[:node_rows, :], preferred_element_type=jnp.float32
        ).astype(jnp.bfloat16)
        pre = (
            jnp.dot(joined[...], w_in_ref[...], preferred_element_type=jnp.float32) + b_in_ref[...]
        )
        active = silu(pre).astype(jnp.bfloat16)
        output = (
            jnp.dot(active, w_out_ref[...], preferred_element_type=jnp.float32) + b_out_ref[...]
        )
        update = normalize(output, gain_ref[...], shift_ref[...])
        position = start + lax.broadcasted_iota(jnp.int32, (EDGE_BLOCK, 1), 0)
        message = jnp.where(position < count_ref[0], update, 0.0)
        edges_out_ref[here, :] = (latent.astype(jnp.float32) + message).astype(jnp.bfloat16)
        sent[here, :] = message.astype(jnp.bfloat16)
        return carry

    lax.fori_loop(0, rows // EDGE_BLOCK, edge_block, 0)

    share = hot_sum.shape[0]

    def sum_block(j, carry):
        start = pl.multiple_of(j * share, share)
        node = start + lax.broadcasted_iota(jnp.int32, (share, LANES), 0)
        for k in range(rows // LANES):
            ids = jnp.broadcast_to(receivers_ref[k : k + 1, :], (share, LANES))
            hot_sum[:, k * LANES : (k + 1) * LANES] = jnp.where(node == ids, 1.0, 0.0).astype(
                jnp.bfloat16
            )
        sums_ref[pl.ds(start, share), :] = jnp.dot(
            hot_sum[...], sent[...], preferred_element_type=jnp.float32
        ).astype(jnp.bfloat16)
        return carry

    lax.fori_loop(0, node_rows // share, sum_block, 0)


def edge_stage(table, edges, senders, receivers, edge_count, w_in, b_in, w_out, b_out, gain, shift, node_rows):
    rows, columns = edges.shape
    vmem = pl.BlockSpec(memory_space=pltpu.VMEM)
    return pl.pallas_call(
        edge_kernel,
        out_shape=(
            jax.ShapeDtypeStruct((rows, columns), jnp.bfloat16),
            jax.ShapeDtypeStruct((node_rows, columns), jnp.bfloat16),
        ),
        in_specs=[pl.BlockSpec(memory_space=pltpu.SMEM)] + [vmem] * 10,
        out_specs=(vmem, vmem),
        scratch_shapes=[
            pltpu.VMEM((EDGE_BLOCK, table.shape[0]), jnp.bfloat16),
            pltpu.VMEM((EDGE_BLOCK, node_rows), jnp.bfloat16),
            pltpu.VMEM((512, rows), jnp.bfloat16),
            pltpu.VMEM((EDGE_BLOCK, 3 * columns), jnp.bfloat16),
            pltpu.VMEM((rows, columns), jnp.bfloat16),
        ],
        compiler_params=pltpu.CompilerParams(vmem_limit_bytes=60 * 2**20),
    )(
        edge_count,
        table,
        edges,
        senders.reshape(-1, LANES),
        receivers.reshape(-1, LANES),
        w_in,
        b_in.reshape(1, -1),
        w_out,
        b_out.reshape(1, -1),
        gain.reshape(1, -1),
        shift.reshape(1, -1),
    )


def local(
    nodes,
    edges,
    senders,
    receivers,
    halo_rows,
    coarse_rows,
    edge_count,
    w_edge_in,
    b_edge_in,
    w_edge_out,
    b_edge_out,
    edge_gain,
    edge_shift,
    w_node_in,
    b_node_in,
    w_node_out,
    b_node_out,
    node_gain,
    node_shift,
):
    own_block = collect(nodes, "hidden", 1)
    node_rows = own_block.shape[0]
    columns = own_block.shape[1]
    border_rows = halo_rows.shape[2]
    patches = lax.axis_size("patch")
    outgoing = jnp.concatenate([own_block[halo_rows[0, 0]], own_block[halo_rows[0, 1]]], axis=0)
    bordered = extended(outgoing, (("patch", 0),), border_rows)
    everyone = collect(own_block[:COARSE_DEV], "patch", 0)
    owner_start = jnp.arange(patches, dtype=jnp.int32)[:, None] * COARSE_DEV
    distant = everyone[(owner_start + coarse_rows[0]).reshape(-1)]
    sender_table = jnp.concatenate(
        [own_block, bordered[:border_rows], bordered[3 * border_rows :], distant], axis=0
    )
    edges_out, summed = edge_stage(
        sender_table,
        edges,
        senders,
        receivers,
        edge_count,
        w_edge_in,
        b_edge_in,
        w_edge_out,
        b_edge_out,
        edge_gain,
        edge_shift,
        node_rows,
    )
    aggregated = sent_and_summed(summed, "hidden", 0)
    share_rows = aggregated.shape[0]
    own_rows = lax.dynamic_slice_in_dim(
        own_block, lax.axis_index("hidden") * share_rows, share_rows, 0
    )
    pre_active = jnp.dot(own_rows, w_node_in[:columns], preferred_element_type=jnp.float32)
    pre_active = (
        pre_active
        + jnp.dot(
            aggregated.astype(jnp.bfloat16), w_node_in[columns:], preferred_element_type=jnp.float32
        )
        + b_node_in
    )
    active = jax.nn.silu(pre_active).astype(jnp.bfloat16)
    output = jnp.dot(active, w_node_out, preferred_element_type=jnp.float32) + b_node_out
    update = normalize(output, node_gain, node_shift)
    new_rows = (own_rows.astype(jnp.float32) + update).astype(jnp.bfloat16)
    nodes_out = lax.all_to_all(new_rows, "hidden", split_axis=1, concat_axis=0, tiled=True)
    return (nodes_out, edges_out)


def solution(mesh):
    return jax.shard_map(
        local,
        mesh=mesh,
        in_specs=(
            P("patch", "hidden"),
            P(("patch", "hidden"), None),
            P(("patch", "hidden")),
            P(("patch", "hidden")),
            P("patch", None, None),
            P("patch", None, None),
            P(("patch", "hidden")),
            P(),
            P(),
            P(),
            P(),
            P(),
            P(),
            P(),
            P(),
            P(),
            P(),
            P(),
            P(),
        ),
        out_specs=(P("patch", "hidden"), P(("patch", "hidden"), None)),
        check_vma=False,
    )
```

```python
import jax
import jax.numpy as jnp
from jax import lax
from jax.experimental import pallas as pl
from jax.experimental.pallas import tpu as pltpu
from jax.sharding import PartitionSpec as P

COARSE_DEV = 64
LANES = 128
ROW_BLOCK = 512
CHUNKS = 4
MESH = pl.DeviceIdType.MESH


layer_epsilon = 1e-05

TO_RIGHT, TO_LEFT, RELAY_RIGHT, RELAY_LEFT = 0, 4, 8, 10
FORWARD, BACKWARD, COARSE, PICKED = 12, 16, 20, 21
SLOTS = 24
L_NODES, L_EDGES, L_IN, L_OUT, L_RESULT = 0, 1, 2, 3, 4
LOCALS = 12


def in_blocks(array, dim, count):
    lengths = array.shape
    blocks = array.reshape(*lengths[:dim], count, lengths[dim] // count, *lengths[dim + 1 :])
    return jnp.moveaxis(blocks, dim, 0)


def sent_and_summed(array, axis, dim):
    blocks = in_blocks(array, dim, lax.axis_size(axis))
    arrived = lax.all_to_all(blocks, axis, split_axis=0, concat_axis=0, tiled=True)
    return arrived.astype(jnp.float32).sum(axis=0)


def normalize(output, norm_gain, norm_shift):
    row_mean = jnp.mean(output, axis=1, keepdims=True)
    centered = output - row_mean
    row_var = jnp.mean(jnp.square(centered), axis=1, keepdims=True)
    return centered * lax.rsqrt(row_var + layer_epsilon) * norm_gain + norm_shift


def silu(v):
    half = 0.5 * v
    return half + half * jnp.tanh(half)


def one_hot_rows(ids_ref, out_ref, offset=None):
    rows, width = out_ref.shape
    lane = lax.broadcasted_iota(jnp.int32, (LANES, LANES), 1)

    def block(r, carry):
        line = ids_ref[pl.ds(r, 1), :]
        if offset is not None:
            line = line + offset(r)
        ids = jnp.broadcast_to(line, (LANES, LANES)).T
        here = pl.ds(pl.multiple_of(r * LANES, LANES), LANES)
        for k in range(width // LANES):
            out_ref[here, k * LANES : (k + 1) * LANES] = jnp.where(
                ids == lane + k * LANES, 1.0, 0.0
            ).astype(jnp.bfloat16)
        return carry

    lax.fori_loop(0, rows // LANES, block, 0)


def layer_kernel(
    coarse_dev,
    count_ref,
    nodes_ref,
    edges_ref,
    senders_ref,
    receivers_ref,
    halo_ref,
    coarse_ref,
    w_in_ref,
    b_in_ref,
    w_out_ref,
    b_out_ref,
    gain_ref,
    shift_ref,
    edges_out_ref,
    sums_ref,
    own_rows_ref,
    table,
    outgoing,
    everyone,
    hot_halo,
    hot_send,
    hot_recv,
    hot_pick,
    send_rows,
    recv_rows,
    pre,
    edges,
    sent,
    w_in,
    w_out,
    send_sem,
    recv_sem,
    local_sem,
):
    p, h = lax.axis_index("patch"), lax.axis_index("hidden")
    patches, shards = lax.axis_size("patch"), lax.axis_size("hidden")
    right, left, far = (lax.rem(h + s, shards) for s in (1, shards - 1, 2))
    after, before = lax.rem(p + 1, patches), lax.rem(p + patches - 1, patches)
    node_rows = nodes_ref.shape[0]
    edge_rows, columns = edges_ref.shape
    border = outgoing.shape[1] // 2
    chunk = node_rows // CHUNKS
    block = min(ROW_BLOCK, edge_rows)

    def copy_to(source, target, slot, q, g):
        return pltpu.make_async_remote_copy(
            src_ref=source,
            dst_ref=target,
            send_sem=send_sem.at[slot],
            recv_sem=recv_sem.at[slot],
            device_id={"patch": q, "hidden": g},
            device_id_type=MESH,
        )

    def rows_of(part, k):
        return table.at[part, pl.ds(k * chunk, chunk), :]

    barrier = pltpu.get_barrier_semaphore()

    def greet(j, carry):
        pl.semaphore_signal(
            barrier,
            inc=1,
            device_id={"patch": lax.rem(p + j, patches), "hidden": h},
            device_id_type=MESH,
        )
        return carry

    for g in (right, left, far):
        pl.semaphore_signal(barrier, inc=1, device_id={"patch": p, "hidden": g}, device_id_type=MESH)
    lax.fori_loop(1, patches, greet, 0)

    nodes_in = pltpu.make_async_copy(
        nodes_ref, table.at[h, pl.ds(0, node_rows), :], local_sem.at[L_NODES]
    )
    edges_in = pltpu.make_async_copy(edges_ref, edges, local_sem.at[L_EDGES])
    w_in_in = pltpu.make_async_copy(w_in_ref, w_in, local_sem.at[L_IN])
    w_out_in = pltpu.make_async_copy(w_out_ref, w_out, local_sem.at[L_OUT])
    for c in (nodes_in, edges_in, w_in_in, w_out_in):
        c.start()

    one_hot_rows(halo_ref, hot_halo)
    pl.semaphore_wait(barrier, patches + 2)
    nodes_in.wait()

    to_right = [copy_to(rows_of(h, k), rows_of(h, k), TO_RIGHT + k, p, right) for k in range(CHUNKS)]
    to_left = [copy_to(rows_of(h, k), rows_of(h, k), TO_LEFT + k, p, left) for k in range(CHUNKS)]
    for a, b in ((0, 2), (1, 3), (2, 0), (3, 1)):
        to_right[a].start()
        to_left[b].start()

    slot_rows = pl.ds(pl.multiple_of(p * coarse_dev, coarse_dev), coarse_dev)
    own_coarse = table.at[h, pl.ds(0, coarse_dev), :]

    def share(j, carry):
        copy_to(own_coarse, everyone.at[slot_rows, :], COARSE, lax.rem(p + j, patches), h).start()
        return carry

    lax.fori_loop(1, patches, share, 0)
    everyone[slot_rows, :] = own_coarse[...]

    border_blocks = 2 * border // min(ROW_BLOCK, 2 * border)

    def send_halo(parts, names):
        width = len(parts) * LANES
        source = jnp.concatenate([table[c, :node_rows, :] for c in parts], axis=1)
        size = 2 * border // border_blocks

        def piece(i, carry):
            here = pl.ds(pl.multiple_of(i * size, size), size)
            result = jnp.dot(
                hot_halo[here, :],
                jnp.concatenate([table[c, :node_rows, :] for c in parts], axis=1),
                preferred_element_type=jnp.float32,
            ).astype(jnp.bfloat16)
            for n, name in enumerate(names):
                outgoing[name, here, :] = result[:, n * LANES : (n + 1) * LANES]
            return carry

        lax.fori_loop(0, border_blocks, piece, 0)
        copies = []
        for part, name in zip(parts, names):
            back = copy_to(
                outgoing.at[name, pl.ds(0, border), :],
                table.at[part, pl.ds(node_rows + border, border), :],
                BACKWARD + name,
                before,
                h,
            )
            forth = copy_to(
                outgoing.at[name, pl.ds(border, border), :],
                table.at[part, pl.ds(node_rows, border), :],
                FORWARD + name,
                after,
                h,
            )
            back.start()
            forth.start()
            copies += [back, forth]
        return copies

    halos = {}
    halos[0] = send_halo((h,), (0,))

    edges_in.wait()
    w_in_in.wait()

    def self_block(i, carry):
        here = pl.ds(pl.multiple_of(i * block, block), block)
        pre[here, :] = (
            jnp.dot(edges[here, :], w_in[:columns, :], preferred_element_type=jnp.float32)
            + b_in_ref[...]
        )
        return carry

    lax.fori_loop(0, edge_rows // block, self_block, 0)

    one_hot_rows(receivers_ref, hot_recv)
    per_slot = hot_pick.shape[0] // patches
    spot = lax.broadcasted_iota(jnp.int32, (1, LANES), 1)
    one_hot_rows(
        coarse_ref, hot_pick, lambda r: lax.div(r * LANES + spot, per_slot) * coarse_dev
    )

    def from_left(k):
        return copy_to(rows_of(left, k), rows_of(left, k), TO_RIGHT + k, p, right)

    def from_right(k):
        return copy_to(rows_of(right, k), rows_of(right, k), TO_LEFT + k, p, left)

    relay_right = [copy_to(rows_of(left, k), rows_of(left, k), RELAY_RIGHT + k, p, right) for k in (0, 1)]
    relay_left = [copy_to(rows_of(right, k + 2), rows_of(right, k + 2), RELAY_LEFT + k, p, left) for k in (0, 1)]
    for k in (0, 1):
        from_left(k).wait_recv()
        relay_right[k].start()
        from_right(k + 2).wait_recv()
        relay_left[k].start()

    peers = (patches - 1) * coarse_dev
    all_coarse = copy_to(
        everyone.at[pl.ds(0, peers), :], everyone.at[pl.ds(0, peers), :], COARSE, after, h
    )
    all_coarse.wait_recv()
    first_picked = node_rows + 2 * border
    picked_rows = hot_pick.shape[0]
    picked = table.at[h, pl.ds(first_picked, picked_rows), :]
    table[h, first_picked : first_picked + picked_rows, :] = jnp.dot(
        hot_pick[...], everyone[...], preferred_element_type=jnp.float32
    ).astype(jnp.bfloat16)
    pick_copies = [copy_to(picked, picked, PICKED + n, p, g) for n, g in enumerate((right, left, far))]
    for c in pick_copies:
        c.start()

    one_hot_rows(senders_ref, hot_send)

    for k in (2, 3):
        from_left(k).wait_recv()
        from_right(k - 2).wait_recv()
    halos[1] = send_halo((left, right), (1, 2))

    def gather(hot, low, high, parts, into, add):
        def piece(i, carry):
            here = pl.ds(pl.multiple_of(i * block, block), block)
            result = jnp.dot(
                hot[here, low:high],
                jnp.concatenate([table[c, low:high, :] for c in parts], axis=1),
                preferred_element_type=jnp.float32,
            ).astype(jnp.bfloat16)
            for n, c in enumerate(parts):
                value = result[:, n * LANES : (n + 1) * LANES]
                into[c, here, :] = into[c, here, :] + value if add else value
            return carry

        lax.fori_loop(0, edge_rows // block, piece, 0)

    gather(hot_recv, 0, node_rows, (left, right), recv_rows, False)
    gather(hot_send, 0, node_rows, (left, right), send_rows, False)

    for k in (0, 1):
        copy_to(rows_of(far, k), rows_of(far, k), RELAY_RIGHT + k, p, right).wait_recv()
        copy_to(rows_of(far, k + 2), rows_of(far, k + 2), RELAY_LEFT + k, p, left).wait_recv()
    halos[2] = send_halo((far,), (3,))

    gather(hot_recv, 0, node_rows, (h, far), recv_rows, False)
    gather(hot_send, 0, node_rows, (h, far), send_rows, False)
    total_rows = table.shape[1]
    for c in halos[1]:
        c.wait_recv()
    for n, g in enumerate((left, right, far)):
        landed = table.at[g, pl.ds(first_picked, picked_rows), :]
        copy_to(landed, landed, PICKED + n, p, right).wait_recv()
    gather(hot_send, node_rows, total_rows, (left, right), send_rows, True)
    for c in halos[0] + halos[2]:
        c.wait_recv()
    gather(hot_send, node_rows, total_rows, (h, far), send_rows, True)

    w_out_in.wait()

    def edge_block(i, carry):
        start = pl.multiple_of(i * block, block)
        here = pl.ds(start, block)
        gathered = jnp.concatenate(
            [send_rows[c, here, :] for c in range(columns // LANES)]
            + [recv_rows[c, here, :] for c in range(columns // LANES)],
            axis=1,
        )
        value = pre[here, :] + jnp.dot(
            gathered, w_in[columns:, :], preferred_element_type=jnp.float32
        )
        active = silu(value).astype(jnp.bfloat16)
        output = jnp.dot(active, w_out[...], preferred_element_type=jnp.float32) + b_out_ref[...]
        update = normalize(output, gain_ref[...], shift_ref[...])
        position = start + lax.broadcasted_iota(jnp.int32, (block, 1), 0)
        message = jnp.where(position < count_ref[0], update, 0.0)
        sent[here, :] = message.astype(jnp.bfloat16)
        edges[here, :] = (edges[here, :].astype(jnp.float32) + message).astype(jnp.bfloat16)
        return carry

    lax.fori_loop(0, edge_rows // block, edge_block, 0)
    edges_done = pltpu.make_async_copy(edges, edges_out_ref, local_sem.at[L_RESULT])
    edges_done.start()

    share_rows = node_rows // shards

    def sum_block(j, carry):
        start = pl.multiple_of(j * share_rows, share_rows)
        node = start + lax.broadcasted_iota(jnp.int32, (share_rows, LANES), 0)
        for k in range(edge_rows // LANES):
            ids = jnp.broadcast_to(receivers_ref[k : k + 1, :], (share_rows, LANES))
            hot_recv[:share_rows, k * LANES : (k + 1) * LANES] = jnp.where(
                node == ids, 1.0, 0.0
            ).astype(jnp.bfloat16)
        sums_ref[pl.ds(start, share_rows), :] = jnp.dot(
            hot_recv[:share_rows, :edge_rows], sent[...], preferred_element_type=jnp.float32
        ).astype(jnp.bfloat16)
        return carry

    lax.fori_loop(0, shards, sum_block, 0)
    mine = pl.ds(pl.multiple_of(h * share_rows, share_rows), share_rows)
    for c in range(columns // LANES):
        own_rows_ref[:, c * LANES : (c + 1) * LANES] = table[c, mine, :]

    for c in to_right + to_left + relay_right + relay_left + pick_copies:
        c.wait_send()
    for c in halos[0] + halos[1] + halos[2]:
        c.wait_send()
    all_coarse.wait_send()
    edges_done.wait()


def layer_stage(nodes, edges, senders, receivers, halo_rows, coarse_rows, edge_count, w_in, b_in, w_out, b_out, gain, shift):
    edge_rows, columns = edges.shape
    node_rows = nodes.shape[0]
    border = halo_rows.shape[2]
    picked = coarse_rows.shape[1] * coarse_rows.shape[2]
    total = node_rows + 2 * border + picked
    shards = lax.axis_size("hidden")
    patches = lax.axis_size("patch")
    vmem = pl.BlockSpec(memory_space=pltpu.VMEM)
    smem = pl.BlockSpec(memory_space=pltpu.SMEM)
    far_away = pl.BlockSpec(memory_space=pl.ANY)
    bf16 = jnp.bfloat16
    parts = columns // LANES
    return pl.pallas_call(
        lambda *refs: layer_kernel(COARSE_DEV, *refs),
        out_shape=(
            jax.ShapeDtypeStruct((edge_rows, columns), bf16),
            jax.ShapeDtypeStruct((node_rows, columns), bf16),
            jax.ShapeDtypeStruct((node_rows // shards, columns), bf16),
        ),
        in_specs=[smem, far_away, far_away, vmem, vmem, vmem, vmem, far_away, vmem, far_away, vmem, vmem, vmem],
        out_specs=(far_away, vmem, vmem),
        scratch_shapes=[
            pltpu.VMEM((parts, total, LANES), bf16),
            pltpu.VMEM((parts, 2 * border, LANES), bf16),
            pltpu.VMEM((patches * COARSE_DEV, LANES), bf16),
            pltpu.VMEM((2 * border, node_rows), bf16),
            pltpu.VMEM((edge_rows, total), bf16),
            pltpu.VMEM((edge_rows, node_rows), bf16),
            pltpu.VMEM((picked, patches * COARSE_DEV), bf16),
            pltpu.VMEM((parts, edge_rows, LANES), bf16),
            pltpu.VMEM((parts, edge_rows, LANES), bf16),
            pltpu.VMEM((edge_rows, columns), jnp.float32),
            pltpu.VMEM((edge_rows, columns), bf16),
            pltpu.VMEM((edge_rows, columns), bf16),
            pltpu.VMEM(w_in.shape, bf16),
            pltpu.VMEM(w_out.shape, bf16),
            pltpu.SemaphoreType.DMA((SLOTS,)),
            pltpu.SemaphoreType.DMA((SLOTS,)),
            pltpu.SemaphoreType.DMA((LOCALS,)),
        ],
        compiler_params=pltpu.CompilerParams(
            vmem_limit_bytes=67043328, collective_id=0, has_side_effects=True
        ),
    )(
        edge_count,
        nodes,
        edges,
        senders.reshape(-1, LANES),
        receivers.reshape(-1, LANES),
        halo_rows.reshape(-1, LANES),
        coarse_rows.reshape(-1, LANES),
        w_in,
        b_in.reshape(1, -1),
        w_out,
        b_out.reshape(1, -1),
        gain.reshape(1, -1),
        shift.reshape(1, -1),
    )


def local(
    nodes,
    edges,
    senders,
    receivers,
    halo_rows,
    coarse_rows,
    edge_count,
    w_edge_in,
    b_edge_in,
    w_edge_out,
    b_edge_out,
    edge_gain,
    edge_shift,
    w_node_in,
    b_node_in,
    w_node_out,
    b_node_out,
    node_gain,
    node_shift,
):
    columns = edges.shape[1]
    edges_out, summed, own_rows = layer_stage(
        nodes,
        edges,
        senders,
        receivers,
        halo_rows,
        coarse_rows,
        edge_count,
        w_edge_in,
        b_edge_in,
        w_edge_out,
        b_edge_out,
        edge_gain,
        edge_shift,
    )
    aggregated = sent_and_summed(summed, "hidden", 0)
    pre_active = jnp.dot(own_rows, w_node_in[:columns], preferred_element_type=jnp.float32)
    pre_active = (
        pre_active
        + jnp.dot(
            aggregated.astype(jnp.bfloat16), w_node_in[columns:], preferred_element_type=jnp.float32
        )
        + b_node_in
    )
    active = jax.nn.silu(pre_active).astype(jnp.bfloat16)
    output = jnp.dot(active, w_node_out, preferred_element_type=jnp.float32) + b_node_out
    update = normalize(output, node_gain, node_shift)
    new_rows = (own_rows.astype(jnp.float32) + update).astype(jnp.bfloat16)
    nodes_out = lax.all_to_all(new_rows, "hidden", split_axis=1, concat_axis=0, tiled=True)
    return (nodes_out, edges_out)


def solution(mesh):
    return jax.shard_map(
        local,
        mesh=mesh,
        in_specs=(
            P("patch", "hidden"),
            P(("patch", "hidden"), None),
            P(("patch", "hidden")),
            P(("patch", "hidden")),
            P("patch", None, None),
            P("patch", None, None),
            P(("patch", "hidden")),
            *([P()] * 12),
        ),
        out_specs=(P("patch", "hidden"), P(("patch", "hidden"), None)),
        check_vma=False,
    )
```

```python
import jax
import jax.numpy as jnp
from jax import lax
from jax.experimental import pallas as pl
from jax.experimental.pallas import tpu as pltpu
from jax.sharding import PartitionSpec as P

COARSE_DEV = 64
LANES = 128
ROW_BLOCK = 512
CHUNKS = 4
MESH = pl.DeviceIdType.MESH


layer_epsilon = 1e-05

TO_RIGHT, TO_LEFT, RELAY_RIGHT, RELAY_LEFT = 0, 4, 8, 10
FORWARD, BACKWARD, COARSE, PICKED = 12, 16, 20, 21
PIECES = 2
PASS_RIGHT, PASS_LEFT = 24, 26
PLAIN_RIGHT, PLAIN_LEFT = 28, 30
SUM_RIGHT, SUM_LEFT = 32, 34
NEW = 36
SLOTS = NEW + 6 * PIECES
L_NODES, L_EDGES, L_IN, L_OUT, L_NODE_IN, L_NODE_OUT, L_RESULT, L_OWN = 0, 1, 2, 3, 4, 5, 6, 7
LOCALS = 8


def normalize(output, norm_gain, norm_shift):
    row_mean = jnp.mean(output, axis=1, keepdims=True)
    centered = output - row_mean
    row_var = jnp.mean(jnp.square(centered), axis=1, keepdims=True)
    return centered * lax.rsqrt(row_var + layer_epsilon) * norm_gain + norm_shift


def silu(v):
    half = 0.5 * v
    return half + half * jnp.tanh(half)


def one_hot_rows(line_of, out_ref):
    rows, width = out_ref.shape
    lane = lax.broadcasted_iota(jnp.int32, (LANES, LANES), 1)

    def block(r, carry):
        ids = jnp.broadcast_to(line_of(r), (LANES, LANES)).T
        here = pl.ds(pl.multiple_of(r * LANES, LANES), LANES)
        for k in range(width // LANES):
            out_ref[here, k * LANES : (k + 1) * LANES] = jnp.where(
                ids == lane + k * LANES, 1.0, 0.0
            ).astype(jnp.bfloat16)
        return carry

    lax.fori_loop(0, rows // LANES, block, 0)


def layer_kernel(
    coarse_dev,
    count_ref,
    nodes_ref,
    edges_ref,
    senders_ref,
    receivers_ref,
    halo_ref,
    coarse_ref,
    w_in_ref,
    b_in_ref,
    w_out_ref,
    b_out_ref,
    gain_ref,
    shift_ref,
    w_node_in_ref,
    b_node_in_ref,
    w_node_out_ref,
    b_node_out_ref,
    node_gain_ref,
    node_shift_ref,
    nodes_out_ref,
    edges_out_ref,
    table,
    outgoing,
    everyone,
    hot_halo,
    hot_send,
    hot_recv,
    hot_pick,
    send_rows,
    recv_rows,
    pre,
    edges,
    sent,
    w_in,
    w_out,
    w_node_in,
    w_node_out,
    sums,
    passed,
    plain,
    summed,
    pre_node,
    new,
    send_sem,
    recv_sem,
    local_sem,
):
    p, h = lax.axis_index("patch"), lax.axis_index("hidden")
    patches, shards = lax.axis_size("patch"), lax.axis_size("hidden")
    right, left, far = (lax.rem(h + s, shards) for s in (1, shards - 1, 2))
    after, before = lax.rem(p + 1, patches), lax.rem(p + patches - 1, patches)
    node_rows = nodes_ref.shape[0]
    edge_rows, columns = edges_ref.shape
    border = outgoing.shape[1] // 2
    chunk = node_rows // CHUNKS
    block = min(ROW_BLOCK, edge_rows)

    def copy_to(source, target, slot, q, g):
        return pltpu.make_async_remote_copy(
            src_ref=source,
            dst_ref=target,
            send_sem=send_sem.at[slot],
            recv_sem=recv_sem.at[slot],
            device_id={"patch": q, "hidden": g},
            device_id_type=MESH,
        )

    def rows_of(part, k):
        return table.at[part, pl.ds(k * chunk, chunk), :]

    barrier = pltpu.get_barrier_semaphore()

    def greet(j, carry):
        pl.semaphore_signal(
            barrier,
            inc=1,
            device_id={"patch": lax.rem(p + j, patches), "hidden": h},
            device_id_type=MESH,
        )
        return carry

    for g in (right, left, far):
        pl.semaphore_signal(barrier, inc=1, device_id={"patch": p, "hidden": g}, device_id_type=MESH)
    lax.fori_loop(1, patches, greet, 0)

    nodes_in = pltpu.make_async_copy(
        nodes_ref, table.at[h, pl.ds(0, node_rows), :], local_sem.at[L_NODES]
    )
    edges_in = pltpu.make_async_copy(edges_ref, edges, local_sem.at[L_EDGES])
    w_in_in = pltpu.make_async_copy(w_in_ref, w_in, local_sem.at[L_IN])
    w_out_in = pltpu.make_async_copy(w_out_ref, w_out, local_sem.at[L_OUT])
    w_node_in_in = pltpu.make_async_copy(w_node_in_ref, w_node_in, local_sem.at[L_NODE_IN])
    w_node_out_in = pltpu.make_async_copy(w_node_out_ref, w_node_out, local_sem.at[L_NODE_OUT])
    for c in (nodes_in, edges_in, w_in_in, w_out_in, w_node_in_in, w_node_out_in):
        c.start()

    lines = border // LANES

    def halo_line(r):
        side, place = lax.div(r, lines), lax.rem(r, lines)
        both = halo_ref[0, :, pl.ds(pl.multiple_of(place * LANES, LANES), LANES)]
        return jnp.where(side == 0, both[:1], both[1:])

    one_hot_rows(halo_line, hot_halo)
    pl.semaphore_wait(barrier, patches + 2)
    nodes_in.wait()

    to_right = [copy_to(rows_of(h, k), rows_of(h, k), TO_RIGHT + k, p, right) for k in range(CHUNKS)]
    to_left = [copy_to(rows_of(h, k), rows_of(h, k), TO_LEFT + k, p, left) for k in range(CHUNKS)]
    for a, b in ((0, 2), (1, 3), (2, 0), (3, 1)):
        to_right[a].start()
        to_left[b].start()

    slot_rows = pl.ds(pl.multiple_of(p * coarse_dev, coarse_dev), coarse_dev)
    own_coarse = table.at[h, pl.ds(0, coarse_dev), :]

    def share(j, carry):
        copy_to(own_coarse, everyone.at[slot_rows, :], COARSE, lax.rem(p + j, patches), h).start()
        return carry

    lax.fori_loop(1, patches, share, 0)
    everyone[slot_rows, :] = own_coarse[...]

    border_blocks = 2 * border // min(ROW_BLOCK, 2 * border)

    def send_halo(parts, names):
        width = len(parts) * LANES
        source = jnp.concatenate([table[c, :node_rows, :] for c in parts], axis=1)
        size = 2 * border // border_blocks

        def piece(i, carry):
            here = pl.ds(pl.multiple_of(i * size, size), size)
            result = jnp.dot(
                hot_halo[here, :],
                jnp.concatenate([table[c, :node_rows, :] for c in parts], axis=1),
                preferred_element_type=jnp.float32,
            ).astype(jnp.bfloat16)
            for n, name in enumerate(names):
                outgoing[name, here, :] = result[:, n * LANES : (n + 1) * LANES]
            return carry

        lax.fori_loop(0, border_blocks, piece, 0)
        copies = []
        for part, name in zip(parts, names):
            back = copy_to(
                outgoing.at[name, pl.ds(0, border), :],
                table.at[part, pl.ds(node_rows + border, border), :],
                BACKWARD + name,
                before,
                h,
            )
            forth = copy_to(
                outgoing.at[name, pl.ds(border, border), :],
                table.at[part, pl.ds(node_rows, border), :],
                FORWARD + name,
                after,
                h,
            )
            back.start()
            forth.start()
            copies += [back, forth]
        return copies

    halos = {}
    halos[0] = send_halo((h,), (0,))

    edges_in.wait()
    w_in_in.wait()

    def self_block(i, carry):
        here = pl.ds(pl.multiple_of(i * block, block), block)
        pre[here, :] = (
            jnp.dot(edges[here, :], w_in[:columns, :], preferred_element_type=jnp.float32)
            + b_in_ref[...]
        )
        return carry

    lax.fori_loop(0, edge_rows // block, self_block, 0)

    one_hot_rows(lambda r: receivers_ref[pl.ds(r, 1), :], hot_recv)
    per_slot = hot_pick.shape[0] // patches
    first_picked = node_rows + 2 * border
    owner = lax.broadcasted_iota(jnp.int32, (patches, LANES), 0) * coarse_dev
    spot = lax.broadcasted_iota(jnp.int32, (patches, LANES), 1)
    for k in range(per_slot):
        wanted = jnp.broadcast_to(coarse_ref[0, :, k : k + 1], (patches, LANES)) + owner
        for b in range(hot_pick.shape[1] // LANES):
            hot_pick[k * patches : (k + 1) * patches, b * LANES : (b + 1) * LANES] = jnp.where(
                wanted == spot + b * LANES, 1.0, 0.0
            ).astype(jnp.bfloat16)

    def from_left(k):
        return copy_to(rows_of(left, k), rows_of(left, k), TO_RIGHT + k, p, right)

    def from_right(k):
        return copy_to(rows_of(right, k), rows_of(right, k), TO_LEFT + k, p, left)

    relay_right = [copy_to(rows_of(left, k), rows_of(left, k), RELAY_RIGHT + k, p, right) for k in (0, 1)]
    relay_left = [copy_to(rows_of(right, k + 2), rows_of(right, k + 2), RELAY_LEFT + k, p, left) for k in (0, 1)]
    for k in (0, 1):
        from_left(k).wait_recv()
        relay_right[k].start()
        from_right(k + 2).wait_recv()
        relay_left[k].start()

    peers = (patches - 1) * coarse_dev
    all_coarse = copy_to(
        everyone.at[pl.ds(0, peers), :], everyone.at[pl.ds(0, peers), :], COARSE, after, h
    )
    all_coarse.wait_recv()
    picked_rows = hot_pick.shape[0]
    picked = table.at[h, pl.ds(first_picked, picked_rows), :]
    table[h, first_picked : first_picked + picked_rows, :] = jnp.dot(
        hot_pick[...], everyone[...], preferred_element_type=jnp.float32
    ).astype(jnp.bfloat16)
    pick_copies = [copy_to(picked, picked, PICKED + n, p, g) for n, g in enumerate((right, left, far))]
    for c in pick_copies:
        c.start()

    def sender_line(r):
        code = senders_ref[pl.ds(r, 1), :]
        slot = code - first_picked
        moved = lax.rem(slot, per_slot) * patches + lax.div(slot, per_slot)
        return jnp.where(slot >= 0, first_picked + moved, code)

    one_hot_rows(sender_line, hot_send)

    for k in (2, 3):
        from_left(k).wait_recv()
        from_right(k - 2).wait_recv()
    halos[1] = send_halo((left, right), (1, 2))

    def gather(hot, low, high, parts, into, add):
        def piece(i, carry):
            here = pl.ds(pl.multiple_of(i * block, block), block)
            result = jnp.dot(
                hot[here, low:high],
                jnp.concatenate([table[c, low:high, :] for c in parts], axis=1),
                preferred_element_type=jnp.float32,
            ).astype(jnp.bfloat16)
            for n, c in enumerate(parts):
                value = result[:, n * LANES : (n + 1) * LANES]
                into[c, here, :] = into[c, here, :] + value if add else value
            return carry

        lax.fori_loop(0, edge_rows // block, piece, 0)

    gather(hot_recv, 0, node_rows, (left, right), recv_rows, False)
    gather(hot_send, 0, node_rows, (left, right), send_rows, False)

    for k in (0, 1):
        copy_to(rows_of(far, k), rows_of(far, k), RELAY_RIGHT + k, p, right).wait_recv()
        copy_to(rows_of(far, k + 2), rows_of(far, k + 2), RELAY_LEFT + k, p, left).wait_recv()
    halos[2] = send_halo((far,), (3,))

    gather(hot_recv, 0, node_rows, (h, far), recv_rows, False)
    gather(hot_send, 0, node_rows, (h, far), send_rows, False)
    total_rows = table.shape[1]
    for c in halos[1]:
        c.wait_recv()
    for n, g in enumerate((left, right, far)):
        landed = table.at[g, pl.ds(first_picked, picked_rows), :]
        copy_to(landed, landed, PICKED + n, p, right).wait_recv()
    gather(hot_send, node_rows, total_rows, (left, right), send_rows, True)
    for c in halos[0] + halos[2]:
        c.wait_recv()
    gather(hot_send, node_rows, total_rows, (h, far), send_rows, True)

    w_out_in.wait()

    def edge_block(i, carry):
        start = pl.multiple_of(i * block, block)
        here = pl.ds(start, block)
        gathered = jnp.concatenate(
            [send_rows[c, here, :] for c in range(columns // LANES)]
            + [recv_rows[c, here, :] for c in range(columns // LANES)],
            axis=1,
        )
        value = pre[here, :] + jnp.dot(
            gathered, w_in[columns:, :], preferred_element_type=jnp.float32
        )
        active = silu(value).astype(jnp.bfloat16)
        output = jnp.dot(active, w_out[...], preferred_element_type=jnp.float32) + b_out_ref[...]
        update = normalize(output, gain_ref[...], shift_ref[...])
        position = start + lax.broadcasted_iota(jnp.int32, (block, 1), 0)
        message = jnp.where(position < count_ref[0], update, 0.0)
        sent[here, :] = message.astype(jnp.bfloat16)
        edges[here, :] = (edges[here, :].astype(jnp.float32) + message).astype(jnp.bfloat16)
        return carry

    lax.fori_loop(0, edge_rows // block, edge_block, 0)
    edges_done = pltpu.make_async_copy(edges, edges_out_ref, local_sem.at[L_RESULT])
    edges_done.start()

    share_rows = node_rows // shards
    half = share_rows // 2
    size = half // PIECES

    def sum_at(j):
        node = j * share_rows + lax.broadcasted_iota(jnp.int32, (share_rows, LANES), 0)

        def line(k, carry):
            ids = jnp.broadcast_to(receivers_ref[pl.ds(k, 1), :], (share_rows, LANES))
            hot_recv[:share_rows, pl.ds(pl.multiple_of(k * LANES, LANES), LANES)] = jnp.where(
                node == ids, 1.0, 0.0
            ).astype(jnp.bfloat16)
            return carry

        lax.fori_loop(0, edge_rows // LANES, line, 0)
        sums[j] = jnp.dot(
            hot_recv[:share_rows, :edge_rows], sent[...], preferred_element_type=jnp.float32
        ).astype(jnp.bfloat16)

    def piece_rows(k):
        return pl.ds(k * size, size)

    def piece_copy(source, target, slot, g):
        return copy_to(source, target, slot, p, g)

    sum_at(far)
    ring = []
    for k in range(PIECES):
        ring.append(piece_copy(sums.at[far, piece_rows(k), :], passed.at[0, piece_rows(k), :], PASS_RIGHT + k, right))
        ring.append(piece_copy(sums.at[far, piece_rows(PIECES + k), :], passed.at[1, piece_rows(k), :], PASS_LEFT + k, left))
    for c in ring:
        c.start()
    sum_at(right)
    plain_right = [
        piece_copy(sums.at[right, piece_rows(PIECES + k), :], plain.at[0, piece_rows(k), :], PLAIN_RIGHT + k, right)
        for k in range(PIECES)
    ]
    for c in plain_right:
        c.start()
    sum_at(left)
    plain_left = [
        piece_copy(sums.at[left, piece_rows(k), :], plain.at[1, piece_rows(k), :], PLAIN_LEFT + k, left)
        for k in range(PIECES)
    ]
    for c in plain_left:
        c.start()

    sum_copies = []
    for k in range(PIECES):
        here = piece_rows(k)
        other = piece_rows(PIECES + k)
        piece_copy(passed.at[0, here, :], passed.at[0, here, :], PASS_RIGHT + k, right).wait_recv()
        sums[right, k * size : (k + 1) * size, :] = (
            sums[right, k * size : (k + 1) * size, :].astype(jnp.float32)
            + passed[0, k * size : (k + 1) * size, :].astype(jnp.float32)
        ).astype(jnp.bfloat16)
        c = piece_copy(sums.at[right, here, :], summed.at[0, here, :], SUM_RIGHT + k, right)
        c.start()
        sum_copies.append(c)
        piece_copy(passed.at[1, here, :], passed.at[1, here, :], PASS_LEFT + k, left).wait_recv()
        sums[left, half + k * size : half + (k + 1) * size, :] = (
            sums[left, half + k * size : half + (k + 1) * size, :].astype(jnp.float32)
            + passed[1, k * size : (k + 1) * size, :].astype(jnp.float32)
        ).astype(jnp.bfloat16)
        c = piece_copy(sums.at[left, other, :], summed.at[1, here, :], SUM_LEFT + k, left)
        c.start()
        sum_copies.append(c)

    sum_at(h)
    w_node_in_in.wait()
    w_node_out_in.wait()

    def own_rows(first, count):
        there = pl.ds(pl.multiple_of(h * share_rows + first, count), count)
        return jnp.concatenate([table[c, there, :] for c in range(columns // LANES)], axis=1)

    pre_node[...] = (
        jnp.dot(
            own_rows(0, share_rows), w_node_in[:columns, :], preferred_element_type=jnp.float32
        )
        + b_node_in_ref[...]
    )

    new_copies = []
    home = []
    for k in range(PIECES):
        here = piece_rows(k)
        spans = ((k * size, 0), (half + k * size, 1))
        piece_copy(summed.at[0, here, :], summed.at[0, here, :], SUM_RIGHT + k, right).wait_recv()
        piece_copy(summed.at[1, here, :], summed.at[1, here, :], SUM_LEFT + k, left).wait_recv()
        piece_copy(plain.at[0, here, :], plain.at[0, here, :], PLAIN_RIGHT + k, right).wait_recv()
        piece_copy(plain.at[1, here, :], plain.at[1, here, :], PLAIN_LEFT + k, left).wait_recv()
        gathered = jnp.concatenate(
            [
                (
                    sums[h, first : first + size, :].astype(jnp.float32)
                    + summed[side, k * size : (k + 1) * size, :].astype(jnp.float32)
                    + plain[1 - side, k * size : (k + 1) * size, :].astype(jnp.float32)
                ).astype(jnp.bfloat16)
                for first, side in spans
            ],
            axis=0,
        )
        value = jnp.concatenate([pre_node[first : first + size, :] for first, side in spans], axis=0)
        value = value + jnp.dot(
            gathered, w_node_in[columns:, :], preferred_element_type=jnp.float32
        )
        active = silu(value).astype(jnp.bfloat16)
        output = jnp.dot(active, w_node_out[...], preferred_element_type=jnp.float32) + b_node_out_ref[...]
        update = normalize(output, node_gain_ref[...], node_shift_ref[...])
        old = jnp.concatenate([own_rows(first, size) for first, side in spans], axis=0)
        result = (old.astype(jnp.float32) + update).astype(jnp.bfloat16)
        for c in range(columns // LANES):
            for n, (first, side) in enumerate(spans):
                new[c, first : first + size, :] = result[
                    n * size : (n + 1) * size, c * LANES : (c + 1) * LANES
                ]
        for n, (first, side) in enumerate(spans):
            there = pl.ds(pl.multiple_of(h * share_rows + first, size), size)
            for m, g in enumerate((far, right, left)):
                c = piece_copy(
                    new.at[g, pl.ds(first, size), :],
                    nodes_out_ref.at[there, :],
                    NEW + (k * 2 + n) * 3 + m,
                    g,
                )
                c.start()
                new_copies.append(c)
    share_there = pl.ds(pl.multiple_of(h * share_rows, share_rows), share_rows)
    home = pltpu.make_async_copy(new.at[h], nodes_out_ref.at[share_there, :], local_sem.at[L_OWN])
    home.start()

    for c in to_right + to_left + relay_right + relay_left + pick_copies:
        c.wait_send()
    for c in halos[0] + halos[1] + halos[2]:
        c.wait_send()
    all_coarse.wait_send()
    for c in ring + plain_right + plain_left + sum_copies + new_copies:
        c.wait_send()
    edges_done.wait()
    home.wait()
    for k in range(PIECES):
        for n, first in enumerate((k * size, half + k * size)):
            for m, g in enumerate((far, left, right)):
                there = pl.ds(pl.multiple_of(g * share_rows + first, size), size)
                landed = nodes_out_ref.at[there, :]
                piece_copy(landed, landed, NEW + (k * 2 + n) * 3 + m, right).wait_recv()


def layer_stage(
    nodes,
    edges,
    senders,
    receivers,
    halo_rows,
    coarse_rows,
    edge_count,
    w_edge_in,
    b_edge_in,
    w_edge_out,
    b_edge_out,
    edge_gain,
    edge_shift,
    w_node_in,
    b_node_in,
    w_node_out,
    b_node_out,
    node_gain,
    node_shift,
):
    edge_rows, columns = edges.shape
    node_rows = nodes.shape[0]
    border = halo_rows.shape[2]
    picked = coarse_rows.shape[1] * coarse_rows.shape[2]
    total = node_rows + 2 * border + picked
    shards = lax.axis_size("hidden")
    patches = lax.axis_size("patch")
    share_rows = node_rows // shards
    vmem = pl.BlockSpec(memory_space=pltpu.VMEM)
    smem = pl.BlockSpec(memory_space=pltpu.SMEM)
    far_away = pl.BlockSpec(memory_space=pl.ANY)
    bf16 = jnp.bfloat16
    parts = columns // LANES
    network = [far_away, vmem, far_away, vmem, vmem, vmem]

    def row(v):
        return v.reshape(1, -1)

    return pl.pallas_call(
        lambda *refs: layer_kernel(COARSE_DEV, *refs),
        out_shape=(
            jax.ShapeDtypeStruct(nodes.shape, bf16),
            jax.ShapeDtypeStruct((edge_rows, columns), bf16),
        ),
        in_specs=[smem, far_away, far_away, vmem, vmem, vmem, vmem, *network, *network],
        out_specs=(far_away, far_away),
        scratch_shapes=[
            pltpu.VMEM((parts, total, LANES), bf16),
            pltpu.VMEM((parts, 2 * border, LANES), bf16),
            pltpu.VMEM((patches * COARSE_DEV, LANES), bf16),
            pltpu.VMEM((2 * border, node_rows), bf16),
            pltpu.VMEM((edge_rows, total), bf16),
            pltpu.VMEM((edge_rows, node_rows), bf16),
            pltpu.VMEM((picked, patches * COARSE_DEV), bf16),
            pltpu.VMEM((parts, edge_rows, LANES), bf16),
            pltpu.VMEM((parts, edge_rows, LANES), bf16),
            pltpu.VMEM((edge_rows, columns), jnp.float32),
            pltpu.VMEM((edge_rows, columns), bf16),
            pltpu.VMEM((edge_rows, columns), bf16),
            pltpu.VMEM(w_edge_in.shape, bf16),
            pltpu.VMEM(w_edge_out.shape, bf16),
            pltpu.VMEM(w_node_in.shape, bf16),
            pltpu.VMEM(w_node_out.shape, bf16),
            pltpu.VMEM((shards, share_rows, columns), bf16),
            pltpu.VMEM((2, share_rows // 2, columns), bf16),
            pltpu.VMEM((2, share_rows // 2, columns), bf16),
            pltpu.VMEM((2, share_rows // 2, columns), bf16),
            pltpu.VMEM((share_rows, columns), jnp.float32),
            pltpu.VMEM((parts, share_rows, LANES), bf16),
            pltpu.SemaphoreType.DMA((SLOTS,)),
            pltpu.SemaphoreType.DMA((SLOTS,)),
            pltpu.SemaphoreType.DMA((LOCALS,)),
        ],
        compiler_params=pltpu.CompilerParams(
            vmem_limit_bytes=67043328, collective_id=0, has_side_effects=True
        ),
    )(
        edge_count,
        nodes,
        edges,
        senders.reshape(-1, LANES),
        receivers.reshape(-1, LANES),
        halo_rows,
        coarse_rows,
        w_edge_in,
        row(b_edge_in),
        w_edge_out,
        row(b_edge_out),
        row(edge_gain),
        row(edge_shift),
        w_node_in,
        row(b_node_in),
        w_node_out,
        row(b_node_out),
        row(node_gain),
        row(node_shift),
    )


def solution(mesh):
    return jax.shard_map(
        layer_stage,
        mesh=mesh,
        in_specs=(
            P("patch", "hidden"),
            P(("patch", "hidden"), None),
            P(("patch", "hidden")),
            P(("patch", "hidden")),
            P("patch", None, None),
            P("patch", None, None),
            P(("patch", "hidden")),
            *([P()] * 12),
        ),
        out_specs=(P("patch", "hidden"), P(("patch", "hidden"), None)),
        check_vma=False,
    )
```

```python
import jax
import jax.numpy as jnp
from jax import lax
from jax.experimental import pallas as pl
from jax.experimental.pallas import tpu as pltpu
from jax.sharding import PartitionSpec as P

COARSE_DEV = 64
LANES = 128
ROW_BLOCK = 512
LONG_BLOCK = 1024
CHUNKS = 4
MESH = pl.DeviceIdType.MESH


layer_epsilon = 1e-05

TO_RIGHT, TO_LEFT, RELAY_RIGHT, RELAY_LEFT = 0, 4, 8, 10
FORWARD, BACKWARD, COARSE, PICKED = 12, 16, 20, 21
PIECES = 4
PASS_RIGHT, PASS_LEFT = 24, 24 + PIECES
PLAIN_RIGHT, PLAIN_LEFT = 24 + 2 * PIECES, 24 + 3 * PIECES
SUM_RIGHT, SUM_LEFT = 24 + 4 * PIECES, 24 + 5 * PIECES
NEW = 24 + 6 * PIECES
SLOTS = NEW + 6 * PIECES
L_NODES, L_EDGES, L_IN, L_OUT, L_NODE_IN, L_NODE_OUT, L_RESULT, L_OWN = 0, 1, 2, 3, 4, 5, 6, 7
LOCALS = 8


def normalize(output, norm_gain, norm_shift):
    row_mean = jnp.mean(output, axis=1, keepdims=True)
    centered = output - row_mean
    row_var = jnp.mean(jnp.square(centered), axis=1, keepdims=True)
    return centered * lax.rsqrt(row_var + layer_epsilon) * norm_gain + norm_shift


def silu(v):
    half = 0.5 * v
    return half + half * jnp.tanh(half)


def one_hot(line_of, first, lines, low, high):
    lane = low + lax.broadcasted_iota(jnp.int32, (LANES, LANES), 1)
    rows = []
    for r in range(lines):
        ids = jnp.broadcast_to(line_of(first + r), (LANES, LANES)).T
        rows.append(
            jnp.concatenate(
                [
                    jnp.where(ids == lane + k, 1.0, 0.0).astype(jnp.bfloat16)
                    for k in range(0, high - low, LANES)
                ],
                axis=1,
            )
        )
    return jnp.concatenate(rows, axis=0)


def layer_kernel(
    coarse_dev,
    count_ref,
    nodes_ref,
    edges_ref,
    senders_ref,
    receivers_ref,
    halo_ref,
    coarse_ref,
    w_in_ref,
    b_in_ref,
    w_out_ref,
    b_out_ref,
    gain_ref,
    shift_ref,
    w_node_in_ref,
    b_node_in_ref,
    w_node_out_ref,
    b_node_out_ref,
    node_gain_ref,
    node_shift_ref,
    nodes_out_ref,
    edges_out_ref,
    table,
    outgoing,
    everyone,
    hot_pick,
    send_rows,
    recv_rows,
    pre,
    sent,
    w_in,
    w_out,
    w_node_in,
    w_node_out,
    sums,
    passed,
    plain,
    summed,
    send_sem,
    recv_sem,
    local_sem,
):
    edges = edges_out_ref
    p, h = lax.axis_index("patch"), lax.axis_index("hidden")
    patches, shards = lax.axis_size("patch"), lax.axis_size("hidden")
    right, left, far = (lax.rem(h + s, shards) for s in (1, shards - 1, 2))
    after, before = lax.rem(p + 1, patches), lax.rem(p + patches - 1, patches)
    node_rows = nodes_ref.shape[0]
    edge_rows, columns = edges_ref.shape
    border = outgoing.shape[1] // 2
    chunk = node_rows // CHUNKS
    block = min(ROW_BLOCK, edge_rows)

    def copy_to(source, target, slot, q, g):
        return pltpu.make_async_remote_copy(
            src_ref=source,
            dst_ref=target,
            send_sem=send_sem.at[slot],
            recv_sem=recv_sem.at[slot],
            device_id={"patch": q, "hidden": g},
            device_id_type=MESH,
        )

    def rows_of(part, k):
        return table.at[part, pl.ds(k * chunk, chunk), :]

    barrier = pltpu.get_barrier_semaphore()

    def greet(j, carry):
        pl.semaphore_signal(
            barrier,
            inc=1,
            device_id={"patch": lax.rem(p + j, patches), "hidden": h},
            device_id_type=MESH,
        )
        return carry

    for g in (right, left, far):
        pl.semaphore_signal(barrier, inc=1, device_id={"patch": p, "hidden": g}, device_id_type=MESH)
    lax.fori_loop(1, patches, greet, 0)

    nodes_in = pltpu.make_async_copy(
        nodes_ref, table.at[h, pl.ds(0, node_rows), :], local_sem.at[L_NODES]
    )
    edges_in = pltpu.make_async_copy(edges_ref, edges, local_sem.at[L_EDGES])
    w_in_in = pltpu.make_async_copy(w_in_ref, w_in, local_sem.at[L_IN])
    w_out_in = pltpu.make_async_copy(w_out_ref, w_out, local_sem.at[L_OUT])
    w_node_in_in = pltpu.make_async_copy(w_node_in_ref, w_node_in, local_sem.at[L_NODE_IN])
    w_node_out_in = pltpu.make_async_copy(w_node_out_ref, w_node_out, local_sem.at[L_NODE_OUT])
    for c in (nodes_in, edges_in, w_in_in, w_out_in, w_node_in_in, w_node_out_in):
        c.start()

    lines = border // LANES

    def halo_line(r):
        side, place = lax.div(r, lines), lax.rem(r, lines)
        both = halo_ref[0, :, pl.ds(pl.multiple_of(place * LANES, LANES), LANES)]
        return jnp.where(side == 0, both[:1], both[1:])

    def loop(count, body):
        lax.fori_loop(0, count, lambda i, carry: (body(i), carry)[1], 0)

    pl.semaphore_wait(barrier, patches + 2)
    nodes_in.wait()

    to_right = [copy_to(rows_of(h, k), rows_of(h, k), TO_RIGHT + k, p, right) for k in range(CHUNKS)]
    to_left = [copy_to(rows_of(h, k), rows_of(h, k), TO_LEFT + k, p, left) for k in range(CHUNKS)]
    for a, b in ((0, 1), (1, 0), (2, 3), (3, 2)):
        to_right[a].start()
        to_left[b].start()

    slot_rows = pl.ds(pl.multiple_of(p * coarse_dev, coarse_dev), coarse_dev)
    own_coarse = table.at[h, pl.ds(0, coarse_dev), :]

    def share(j, carry):
        copy_to(own_coarse, everyone.at[slot_rows, :], COARSE, lax.rem(p + j, patches), h).start()
        return carry

    lax.fori_loop(1, patches, share, 0)
    everyone[slot_rows, :] = own_coarse[...]

    long_block = min(LONG_BLOCK, edge_rows, 2 * border)
    long_lines = long_block // LANES
    border_blocks = 2 * border // long_block
    gather_blocks = edge_rows // long_block

    def side(parts, low, high):
        return jnp.concatenate([table[c, low:high, :] for c in parts], axis=1)

    def halo(parts, names, low, high, add):
        def piece(i):
            here = pl.ds(pl.multiple_of(i * long_block, long_block), long_block)
            result = jnp.dot(
                one_hot(halo_line, i * long_lines, long_lines, low, high),
                side(parts, low, high),
                preferred_element_type=jnp.float32,
            ).astype(jnp.bfloat16)
            for n, name in enumerate(names):
                value = result[:, n * LANES : (n + 1) * LANES]
                outgoing[name, here, :] = outgoing[name, here, :] + value if add else value

        loop(border_blocks, piece)

    def send_halo(parts, names):
        copies = []
        for part, name in zip(parts, names):
            back = copy_to(
                outgoing.at[name, pl.ds(0, border), :],
                table.at[part, pl.ds(node_rows + border, border), :],
                BACKWARD + name,
                before,
                h,
            )
            forth = copy_to(
                outgoing.at[name, pl.ds(border, border), :],
                table.at[part, pl.ds(node_rows, border), :],
                FORWARD + name,
                after,
                h,
            )
            back.start()
            forth.start()
            copies += [back, forth]
        return copies

    halos = {}
    edge_lines = edge_rows // LANES
    middle = node_rows // 2
    halo((h,), (0,), 0, node_rows, False)
    halos[0] = send_halo((h,), (0,))

    edges_in.wait()
    w_in_in.wait()

    per_slot = hot_pick.shape[0] // patches
    first_picked = node_rows + 2 * border

    def sender_line(r):
        code = senders_ref[pl.ds(r, 1), :]
        slot = code - first_picked
        moved = lax.rem(slot, per_slot) * patches + lax.div(slot, per_slot)
        return jnp.where(slot >= 0, first_picked + moved, code)

    def self_block(i, carry):
        here = pl.ds(pl.multiple_of(i * block, block), block)
        pre[here, :] = (
            jnp.dot(edges[here, :], w_in[:columns, :], preferred_element_type=jnp.float32)
            + b_in_ref[...]
        )
        return carry

    lax.fori_loop(0, edge_rows // block, self_block, 0)

    owner = lax.broadcasted_iota(jnp.int32, (patches, LANES), 0) * coarse_dev
    spot = lax.broadcasted_iota(jnp.int32, (patches, LANES), 1)
    for k in range(per_slot):
        line = coarse_ref[0, k : k + 1, :]
        wanted = jnp.broadcast_to(line, (LANES, patches)).T + owner
        for b in range(hot_pick.shape[1] // LANES):
            hot_pick[k * patches : (k + 1) * patches, b * LANES : (b + 1) * LANES] = jnp.where(
                wanted == spot + b * LANES, 1.0, 0.0
            ).astype(jnp.bfloat16)

    def from_left(k):
        return copy_to(rows_of(left, k), rows_of(left, k), TO_RIGHT + k, p, right)

    def from_right(k):
        return copy_to(rows_of(right, k), rows_of(right, k), TO_LEFT + k, p, left)

    relay_right = [copy_to(rows_of(left, 2 * k), rows_of(left, 2 * k), RELAY_RIGHT + k, p, right) for k in (0, 1)]
    relay_left = [copy_to(rows_of(right, 2 * k + 1), rows_of(right, 2 * k + 1), RELAY_LEFT + k, p, left) for k in (0, 1)]

    def near_half(k):
        for c in (2 * k, 2 * k + 1):
            from_left(c).wait_recv()
            from_right(c).wait_recv()
        relay_right[k].start()
        relay_left[k].start()

    def far_half(k):
        copy_to(rows_of(far, 2 * k), rows_of(far, 2 * k), RELAY_RIGHT + k, p, right).wait_recv()
        copy_to(rows_of(far, 2 * k + 1), rows_of(far, 2 * k + 1), RELAY_LEFT + k, p, left).wait_recv()

    def gather(line_of, low, high, parts, into, add):
        def piece(i):
            here = pl.ds(pl.multiple_of(i * long_block, long_block), long_block)
            result = jnp.dot(
                one_hot(line_of, i * long_lines, long_lines, low, high),
                side(parts, low, high),
                preferred_element_type=jnp.float32,
            ).astype(jnp.bfloat16)
            for n, c in enumerate(parts):
                value = result[:, n * LANES : (n + 1) * LANES]
                into[c, here, :] = into[c, here, :] + value if add else value

        loop(gather_blocks, piece)

    def receiver_line(r):
        return receivers_ref[pl.ds(r, 1), :]

    near, pair = (left, right), (h, far)
    total_rows = table.shape[1]
    near_half(0)
    halo(near, (1, 2), 0, middle, False)
    gather(receiver_line, 0, middle, near, recv_rows, False)
    gather(sender_line, 0, middle, near, send_rows, False)
    near_half(1)
    peers = (patches - 1) * coarse_dev
    all_coarse = copy_to(
        everyone.at[pl.ds(0, peers), :], everyone.at[pl.ds(0, peers), :], COARSE, after, h
    )
    all_coarse.wait_recv()
    picked_rows = hot_pick.shape[0]
    picked = table.at[h, pl.ds(first_picked, picked_rows), :]
    table[h, first_picked : first_picked + picked_rows, :] = jnp.dot(
        hot_pick[...], everyone[...], preferred_element_type=jnp.float32
    ).astype(jnp.bfloat16)
    pick_copies = [copy_to(picked, picked, PICKED + n, p, g) for n, g in enumerate((right, left, far))]
    for c in pick_copies:
        c.start()

    halo(near, (1, 2), middle, node_rows, True)
    halos[1] = send_halo(near, (1, 2))
    gather(receiver_line, middle, node_rows, near, recv_rows, True)
    gather(sender_line, middle, node_rows, near, send_rows, True)
    far_half(0)
    halo((far,), (3,), 0, middle, False)
    far_half(1)
    halo((far,), (3,), middle, node_rows, True)
    halos[2] = send_halo((far,), (3,))
    gather(receiver_line, 0, node_rows, pair, recv_rows, False)
    gather(sender_line, 0, node_rows, pair, send_rows, False)
    for c in halos[1]:
        c.wait_recv()
    for n, g in enumerate((left, right, far)):
        landed = table.at[g, pl.ds(first_picked, picked_rows), :]
        copy_to(landed, landed, PICKED + n, p, right).wait_recv()
    gather(sender_line, node_rows, total_rows, near, send_rows, True)
    for c in halos[0] + halos[2]:
        c.wait_recv()
    gather(sender_line, node_rows, total_rows, pair, send_rows, True)

    w_out_in.wait()

    def edge_block(i, carry):
        start = pl.multiple_of(i * block, block)
        here = pl.ds(start, block)
        gathered = jnp.concatenate(
            [send_rows[c, here, :] for c in range(columns // LANES)]
            + [recv_rows[c, here, :] for c in range(columns // LANES)],
            axis=1,
        )
        value = pre[here, :] + jnp.dot(
            gathered, w_in[columns:, :], preferred_element_type=jnp.float32
        )
        active = silu(value).astype(jnp.bfloat16)
        output = jnp.dot(active, w_out[...], preferred_element_type=jnp.float32) + b_out_ref[...]
        update = normalize(output, gain_ref[...], shift_ref[...])
        position = start + lax.broadcasted_iota(jnp.int32, (block, 1), 0)
        message = jnp.where(position < count_ref[0], update, 0.0)
        sent[here, :] = message.astype(jnp.bfloat16)
        edges[here, :] = (edges[here, :].astype(jnp.float32) + message).astype(jnp.bfloat16)
        return carry

    lax.fori_loop(0, edge_rows // block, edge_block, 0, unroll=True)

    share_rows = node_rows // shards
    pre_node = pre.at[pl.ds(0, share_rows), :]
    new = send_rows.at[:, pl.ds(0, share_rows), :]
    half = share_rows // 2
    size = half // PIECES

    def sum_at(j):
        node = j * share_rows + lax.broadcasted_iota(jnp.int32, (share_rows, LANES), 0)
        hot = [
            jnp.where(node == jnp.broadcast_to(receivers_ref[k : k + 1, :], node.shape), 1.0, 0.0)
            for k in range(edge_lines)
        ]
        sums[j] = jnp.dot(
            jnp.concatenate([v.astype(jnp.bfloat16) for v in hot], axis=1),
            sent[...],
            preferred_element_type=jnp.float32,
        ).astype(jnp.bfloat16)

    def piece_rows(k):
        return pl.ds(k * size, size)

    def piece_copy(source, target, slot, g):
        return copy_to(source, target, slot, p, g)

    sum_at(far)
    ring = []
    for k in range(PIECES):
        ring.append(piece_copy(sums.at[far, piece_rows(k), :], passed.at[0, piece_rows(k), :], PASS_RIGHT + k, right))
        ring.append(piece_copy(sums.at[far, piece_rows(PIECES + k), :], passed.at[1, piece_rows(k), :], PASS_LEFT + k, left))
    for c in ring:
        c.start()
    sum_at(right)
    plain_right = [
        piece_copy(sums.at[right, piece_rows(PIECES + k), :], plain.at[0, piece_rows(k), :], PLAIN_RIGHT + k, right)
        for k in range(PIECES)
    ]
    for c in plain_right:
        c.start()
    sum_at(left)
    plain_left = [
        piece_copy(sums.at[left, piece_rows(k), :], plain.at[1, piece_rows(k), :], PLAIN_LEFT + k, left)
        for k in range(PIECES)
    ]
    for c in plain_left:
        c.start()

    sum_copies = []
    for k in range(PIECES):
        here = piece_rows(k)
        other = piece_rows(PIECES + k)
        piece_copy(passed.at[0, here, :], passed.at[0, here, :], PASS_RIGHT + k, right).wait_recv()
        sums[right, k * size : (k + 1) * size, :] = (
            sums[right, k * size : (k + 1) * size, :].astype(jnp.float32)
            + passed[0, k * size : (k + 1) * size, :].astype(jnp.float32)
        ).astype(jnp.bfloat16)
        c = piece_copy(sums.at[right, here, :], summed.at[0, here, :], SUM_RIGHT + k, right)
        c.start()
        sum_copies.append(c)
        piece_copy(passed.at[1, here, :], passed.at[1, here, :], PASS_LEFT + k, left).wait_recv()
        sums[left, half + k * size : half + (k + 1) * size, :] = (
            sums[left, half + k * size : half + (k + 1) * size, :].astype(jnp.float32)
            + passed[1, k * size : (k + 1) * size, :].astype(jnp.float32)
        ).astype(jnp.bfloat16)
        c = piece_copy(sums.at[left, other, :], summed.at[1, here, :], SUM_LEFT + k, left)
        c.start()
        sum_copies.append(c)

    sum_at(h)
    w_node_in_in.wait()
    w_node_out_in.wait()

    def own_rows(first, count):
        there = pl.ds(pl.multiple_of(h * share_rows + first, count), count)
        return jnp.concatenate([table[c, there, :] for c in range(columns // LANES)], axis=1)

    pre_node[...] = (
        jnp.dot(
            own_rows(0, share_rows), w_node_in[:columns, :], preferred_element_type=jnp.float32
        )
        + b_node_in_ref[...]
    )

    new_copies = []
    home = []
    for k in range(PIECES):
        here = piece_rows(k)
        spans = ((k * size, 0), (half + k * size, 1))
        piece_copy(summed.at[0, here, :], summed.at[0, here, :], SUM_RIGHT + k, right).wait_recv()
        piece_copy(summed.at[1, here, :], summed.at[1, here, :], SUM_LEFT + k, left).wait_recv()
        piece_copy(plain.at[0, here, :], plain.at[0, here, :], PLAIN_RIGHT + k, right).wait_recv()
        piece_copy(plain.at[1, here, :], plain.at[1, here, :], PLAIN_LEFT + k, left).wait_recv()
        gathered = jnp.concatenate(
            [
                (
                    sums[h, first : first + size, :].astype(jnp.float32)
                    + summed[side, k * size : (k + 1) * size, :].astype(jnp.float32)
                    + plain[1 - side, k * size : (k + 1) * size, :].astype(jnp.float32)
                ).astype(jnp.bfloat16)
                for first, side in spans
            ],
            axis=0,
        )
        value = jnp.concatenate([pre_node[first : first + size, :] for first, side in spans], axis=0)
        value = value + jnp.dot(
            gathered, w_node_in[columns:, :], preferred_element_type=jnp.float32
        )
        active = silu(value).astype(jnp.bfloat16)
        output = jnp.dot(active, w_node_out[...], preferred_element_type=jnp.float32) + b_node_out_ref[...]
        update = normalize(output, node_gain_ref[...], node_shift_ref[...])
        old = jnp.concatenate([own_rows(first, size) for first, side in spans], axis=0)
        result = (old.astype(jnp.float32) + update).astype(jnp.bfloat16)
        for c in range(columns // LANES):
            for n, (first, side) in enumerate(spans):
                new[c, first : first + size, :] = result[
                    n * size : (n + 1) * size, c * LANES : (c + 1) * LANES
                ]
        for n, (first, side) in enumerate(spans):
            there = pl.ds(pl.multiple_of(h * share_rows + first, size), size)
            for m, g in enumerate((far, right, left)):
                c = piece_copy(
                    new.at[g, pl.ds(first, size), :],
                    nodes_out_ref.at[there, :],
                    NEW + (k * 2 + n) * 3 + m,
                    g,
                )
                c.start()
                new_copies.append(c)
    share_there = pl.ds(pl.multiple_of(h * share_rows, share_rows), share_rows)
    nodes_out_ref[share_there, :] = new[h]

    for c in to_right + to_left + relay_right + relay_left + pick_copies:
        c.wait_send()
    for c in halos[0] + halos[1] + halos[2]:
        c.wait_send()
    all_coarse.wait_send()
    for c in ring + plain_right + plain_left + sum_copies + new_copies:
        c.wait_send()
    for k in range(PIECES):
        for n, first in enumerate((k * size, half + k * size)):
            for m, g in enumerate((far, left, right)):
                there = pl.ds(pl.multiple_of(g * share_rows + first, size), size)
                landed = nodes_out_ref.at[there, :]
                piece_copy(landed, landed, NEW + (k * 2 + n) * 3 + m, right).wait_recv()


def layer_stage(
    nodes,
    edges,
    senders,
    receivers,
    halo_rows,
    coarse_rows,
    edge_count,
    w_edge_in,
    b_edge_in,
    w_edge_out,
    b_edge_out,
    edge_gain,
    edge_shift,
    w_node_in,
    b_node_in,
    w_node_out,
    b_node_out,
    node_gain,
    node_shift,
):
    edge_rows, columns = edges.shape
    node_rows = nodes.shape[0]
    border = halo_rows.shape[2]
    picked = coarse_rows.shape[1] * coarse_rows.shape[2]
    total = node_rows + 2 * border + picked
    shards = lax.axis_size("hidden")
    patches = lax.axis_size("patch")
    share_rows = node_rows // shards
    vmem = pl.BlockSpec(memory_space=pltpu.VMEM)
    smem = pl.BlockSpec(memory_space=pltpu.SMEM)
    far_away = pl.BlockSpec(memory_space=pl.ANY)
    bf16 = jnp.bfloat16
    parts = columns // LANES
    network = [far_away, vmem, far_away, vmem, vmem, vmem]

    def row(v):
        return v.reshape(1, -1)

    return pl.pallas_call(
        lambda *refs: layer_kernel(COARSE_DEV, *refs),
        out_shape=(
            pltpu.VMEM(nodes.shape, bf16),
            pltpu.VMEM((edge_rows, columns), bf16),
        ),
        in_specs=[smem, far_away, far_away, vmem, vmem, vmem, vmem, *network, *network],
        out_specs=(vmem, vmem),
        scratch_shapes=[
            pltpu.VMEM((parts, total, LANES), bf16),
            pltpu.VMEM((parts, 2 * border, LANES), bf16),
            pltpu.VMEM((patches * COARSE_DEV, LANES), bf16),
            pltpu.VMEM((picked, patches * COARSE_DEV), bf16),
            pltpu.VMEM((parts, edge_rows, LANES), bf16),
            pltpu.VMEM((parts, edge_rows, LANES), bf16),
            pltpu.VMEM((edge_rows, columns), jnp.float32),
            pltpu.VMEM((edge_rows, columns), bf16),
            pltpu.VMEM(w_edge_in.shape, bf16),
            pltpu.VMEM(w_edge_out.shape, bf16),
            pltpu.VMEM(w_node_in.shape, bf16),
            pltpu.VMEM(w_node_out.shape, bf16),
            pltpu.VMEM((shards, share_rows, columns), bf16),
            pltpu.VMEM((2, share_rows // 2, columns), bf16),
            pltpu.VMEM((2, share_rows // 2, columns), bf16),
            pltpu.VMEM((2, share_rows // 2, columns), bf16),
            pltpu.SemaphoreType.DMA((SLOTS,)),
            pltpu.SemaphoreType.DMA((SLOTS,)),
            pltpu.SemaphoreType.DMA((LOCALS,)),
        ],
        compiler_params=pltpu.CompilerParams(
            vmem_limit_bytes=64000000, collective_id=0, has_side_effects=True
        ),
    )(
        edge_count,
        nodes,
        edges,
        senders.reshape(-1, LANES),
        receivers.reshape(-1, LANES),
        halo_rows,
        jnp.swapaxes(coarse_rows, 1, 2),
        w_edge_in,
        row(b_edge_in),
        w_edge_out,
        row(b_edge_out),
        row(edge_gain),
        row(edge_shift),
        w_node_in,
        row(b_node_in),
        w_node_out,
        row(b_node_out),
        row(node_gain),
        row(node_shift),
    )


def solution(mesh):
    return jax.shard_map(
        layer_stage,
        mesh=mesh,
        in_specs=(
            P("patch", "hidden"),
            P(("patch", "hidden"), None),
            P(("patch", "hidden")),
            P(("patch", "hidden")),
            P("patch", None, None),
            P("patch", None, None),
            P(("patch", "hidden")),
            *([P()] * 12),
        ),
        out_specs=(P("patch", "hidden"), P(("patch", "hidden"), None)),
        check_vma=False,
    )
```

```python
import jax
import jax.numpy as jnp
from jax import lax
from jax.experimental import pallas as pl
from jax.experimental.pallas import tpu as pltpu
from jax.sharding import PartitionSpec as P

COARSE_DEV = 64
LANES = 128
ROW_BLOCK = 512
LONG_BLOCK = 1024
CHUNKS = 4
MESH = pl.DeviceIdType.MESH


layer_epsilon = 1e-05

TO_RIGHT, TO_LEFT, RELAY_RIGHT, RELAY_LEFT = 0, 4, 8, 10
FORWARD, BACKWARD, COARSE, PICKED = 12, 16, 20, 21
PIECES = 4
PASS_RIGHT, PASS_LEFT = 24, 24 + PIECES
PLAIN_RIGHT, PLAIN_LEFT = 24 + 2 * PIECES, 24 + 3 * PIECES
SUM_RIGHT, SUM_LEFT = 24 + 4 * PIECES, 24 + 5 * PIECES
NEW = 24 + 6 * PIECES
SLOTS = NEW + 6 * PIECES
L_NODES, L_EDGES, L_IN, L_OUT, L_NODE_IN, L_NODE_OUT, L_RESULT, L_OWN = 0, 1, 2, 3, 4, 5, 6, 7
LOCALS = 8


def normalize(output, norm_gain, norm_shift):
    row_mean = jnp.mean(output, axis=1, keepdims=True)
    centered = output - row_mean
    row_var = jnp.mean(jnp.square(centered), axis=1, keepdims=True)
    return centered * lax.rsqrt(row_var + layer_epsilon) * norm_gain + norm_shift


def silu(v):
    half = 0.5 * v
    return half + half * jnp.tanh(half)


def one_hot(line_of, first, lines, low, high):
    lane = low + lax.broadcasted_iota(jnp.int32, (LANES, LANES), 1)
    rows = []
    for r in range(lines):
        ids = jnp.broadcast_to(line_of(first + r), (LANES, LANES)).T
        rows.append(
            jnp.concatenate(
                [
                    jnp.where(ids == lane + k, 1.0, 0.0).astype(jnp.bfloat16)
                    for k in range(0, high - low, LANES)
                ],
                axis=1,
            )
        )
    return jnp.concatenate(rows, axis=0)


def layer_kernel(
    coarse_dev,
    count_ref,
    nodes_ref,
    edges_ref,
    senders_ref,
    receivers_ref,
    halo_ref,
    coarse_ref,
    w_in_ref,
    b_in_ref,
    w_out_ref,
    b_out_ref,
    gain_ref,
    shift_ref,
    w_node_in_ref,
    b_node_in_ref,
    w_node_out_ref,
    b_node_out_ref,
    node_gain_ref,
    node_shift_ref,
    nodes_out_ref,
    edges_out_ref,
    table,
    outgoing,
    everyone,
    hot_pick,
    send_rows,
    recv_rows,
    pre,
    sent,
    w_in,
    w_out,
    w_node_in,
    w_node_out,
    sums,
    passed,
    plain,
    summed,
    send_sem,
    recv_sem,
    local_sem,
    known_sem,
):
    edges = edges_out_ref
    p, h = lax.axis_index("patch"), lax.axis_index("hidden")
    patches, shards = lax.axis_size("patch"), lax.axis_size("hidden")
    right, left, far = (lax.rem(h + s, shards) for s in (1, shards - 1, 2))
    after, before = lax.rem(p + 1, patches), lax.rem(p + patches - 1, patches)
    node_rows = nodes_ref.shape[0]
    edge_rows, columns = edges_ref.shape
    border = outgoing.shape[1] // 2
    chunk = node_rows // CHUNKS
    block = min(ROW_BLOCK, edge_rows)

    def copy_to(source, target, slot, q, g):
        return pltpu.make_async_remote_copy(
            src_ref=source,
            dst_ref=target,
            send_sem=send_sem.at[slot],
            recv_sem=recv_sem.at[slot],
            device_id={"patch": q, "hidden": g},
            device_id_type=MESH,
        )

    def rows_of(part, k):
        return table.at[part, pl.ds(k * chunk, chunk), :]

    barrier = pltpu.get_barrier_semaphore()

    def signal(sem, q, g):
        pl.semaphore_signal(sem, inc=1, device_id={"patch": q, "hidden": g}, device_id_type=MESH)

    for g in (right, left, far):
        signal(barrier, p, g)
    for q in (before, after):
        signal(barrier, q, h)

    nodes_in = pltpu.make_async_copy(
        nodes_ref, table.at[h, pl.ds(0, node_rows), :], local_sem.at[L_NODES]
    )
    edges_in = pltpu.make_async_copy(edges_ref, edges, local_sem.at[L_EDGES])
    w_in_in = pltpu.make_async_copy(w_in_ref, w_in, local_sem.at[L_IN])
    w_out_in = pltpu.make_async_copy(w_out_ref, w_out, local_sem.at[L_OUT])
    w_node_in_in = pltpu.make_async_copy(w_node_in_ref, w_node_in, local_sem.at[L_NODE_IN])
    w_node_out_in = pltpu.make_async_copy(w_node_out_ref, w_node_out, local_sem.at[L_NODE_OUT])
    for c in (nodes_in, edges_in, w_in_in, w_out_in, w_node_in_in, w_node_out_in):
        c.start()

    lines = border // LANES

    def halo_line(r):
        side, place = lax.div(r, lines), lax.rem(r, lines)
        both = halo_ref[0, :, pl.ds(pl.multiple_of(place * LANES, LANES), LANES)]
        return jnp.where(side == 0, both[:1], both[1:])

    def loop(count, body):
        lax.fori_loop(0, count, lambda i, carry: (body(i), carry)[1], 0)

    pl.semaphore_wait(barrier, shards + 1)

    def tell(r):
        for q in (lax.rem(p + 2**r, patches), lax.rem(p + patches - 2**r, patches)):
            signal(known_sem.at[r], q, h)

    def learn(r):
        pl.semaphore_wait(known_sem.at[r], 2)
        if r + 1 < rounds:
            tell(r + 1)

    rounds = known_sem.shape[0]
    tell(0)

    def learned(r):
        if r < rounds:
            learn(r)

    nodes_in.wait()

    to_right = [copy_to(rows_of(h, k), rows_of(h, k), TO_RIGHT + k, p, right) for k in range(CHUNKS)]
    to_left = [copy_to(rows_of(h, k), rows_of(h, k), TO_LEFT + k, p, left) for k in range(CHUNKS)]
    for a, b in ((0, 1), (1, 0), (2, 3), (3, 2)):
        to_right[a].start()
        to_left[b].start()


    long_block = min(LONG_BLOCK, edge_rows, 2 * border)
    long_lines = long_block // LANES
    border_blocks = 2 * border // long_block
    gather_blocks = edge_rows // long_block

    def side(parts, low, high):
        return jnp.concatenate([table[c, low:high, :] for c in parts], axis=1)

    def halo(parts, names, low, high, add):
        def piece(i):
            here = pl.ds(pl.multiple_of(i * long_block, long_block), long_block)
            result = jnp.dot(
                one_hot(halo_line, i * long_lines, long_lines, low, high),
                side(parts, low, high),
                preferred_element_type=jnp.float32,
            ).astype(jnp.bfloat16)
            for n, name in enumerate(names):
                value = result[:, n * LANES : (n + 1) * LANES]
                outgoing[name, here, :] = outgoing[name, here, :] + value if add else value

        loop(border_blocks, piece)

    def send_halo(parts, names):
        copies = []
        for part, name in zip(parts, names):
            back = copy_to(
                outgoing.at[name, pl.ds(0, border), :],
                table.at[part, pl.ds(node_rows + border, border), :],
                BACKWARD + name,
                before,
                h,
            )
            forth = copy_to(
                outgoing.at[name, pl.ds(border, border), :],
                table.at[part, pl.ds(node_rows, border), :],
                FORWARD + name,
                after,
                h,
            )
            back.start()
            forth.start()
            copies += [back, forth]
        return copies

    halos = {}
    edge_lines = edge_rows // LANES
    middle = node_rows // 2
    halo((h,), (0,), 0, node_rows, False)
    halos[0] = send_halo((h,), (0,))
    learned(0)

    edges_in.wait()
    w_in_in.wait()

    per_slot = hot_pick.shape[0] // patches
    first_picked = node_rows + 2 * border

    def sender_line(r):
        code = senders_ref[pl.ds(r, 1), :]
        slot = code - first_picked
        moved = lax.rem(slot, per_slot) * patches + lax.div(slot, per_slot)
        return jnp.where(slot >= 0, first_picked + moved, code)

    def self_block(i, carry):
        here = pl.ds(pl.multiple_of(i * block, block), block)
        pre[here, :] = (
            jnp.dot(edges[here, :], w_in[:columns, :], preferred_element_type=jnp.float32)
            + b_in_ref[...]
        )
        return carry

    lax.fori_loop(0, edge_rows // block, self_block, 0)
    learned(1)

    owner = lax.broadcasted_iota(jnp.int32, (patches, LANES), 0) * coarse_dev
    spot = lax.broadcasted_iota(jnp.int32, (patches, LANES), 1)
    for k in range(per_slot):
        line = coarse_ref[0, k : k + 1, :]
        wanted = jnp.broadcast_to(line, (LANES, patches)).T + owner
        for b in range(hot_pick.shape[1] // LANES):
            hot_pick[k * patches : (k + 1) * patches, b * LANES : (b + 1) * LANES] = jnp.where(
                wanted == spot + b * LANES, 1.0, 0.0
            ).astype(jnp.bfloat16)

    def from_left(k):
        return copy_to(rows_of(left, k), rows_of(left, k), TO_RIGHT + k, p, right)

    def from_right(k):
        return copy_to(rows_of(right, k), rows_of(right, k), TO_LEFT + k, p, left)

    relay_right = [copy_to(rows_of(left, 2 * k), rows_of(left, 2 * k), RELAY_RIGHT + k, p, right) for k in (0, 1)]
    relay_left = [copy_to(rows_of(right, 2 * k + 1), rows_of(right, 2 * k + 1), RELAY_LEFT + k, p, left) for k in (0, 1)]

    def near_half(k):
        for c in (2 * k, 2 * k + 1):
            from_left(c).wait_recv()
            from_right(c).wait_recv()
        relay_right[k].start()
        relay_left[k].start()

    def far_half(k):
        copy_to(rows_of(far, 2 * k), rows_of(far, 2 * k), RELAY_RIGHT + k, p, right).wait_recv()
        copy_to(rows_of(far, 2 * k + 1), rows_of(far, 2 * k + 1), RELAY_LEFT + k, p, left).wait_recv()

    def gather(line_of, low, high, parts, into, add):
        def piece(i):
            here = pl.ds(pl.multiple_of(i * long_block, long_block), long_block)
            result = jnp.dot(
                one_hot(line_of, i * long_lines, long_lines, low, high),
                side(parts, low, high),
                preferred_element_type=jnp.float32,
            ).astype(jnp.bfloat16)
            for n, c in enumerate(parts):
                value = result[:, n * LANES : (n + 1) * LANES]
                into[c, here, :] = into[c, here, :] + value if add else value

        loop(gather_blocks, piece)

    def receiver_line(r):
        return receivers_ref[pl.ds(r, 1), :]

    near, pair = (left, right), (h, far)
    total_rows = table.shape[1]
    near_half(0)
    halo(near, (1, 2), 0, middle, False)
    learned(2)
    gather(receiver_line, 0, middle, near, recv_rows, False)
    learned(3)
    slot_rows = pl.ds(pl.multiple_of(p * coarse_dev, coarse_dev), coarse_dev)
    own_coarse = table.at[h, pl.ds(0, coarse_dev), :]

    def share(j, carry):
        copy_to(own_coarse, everyone.at[slot_rows, :], COARSE, lax.rem(p + j, patches), h).start()
        return carry

    lax.fori_loop(1, patches, share, 0)
    everyone[slot_rows, :] = own_coarse[...]

    gather(sender_line, 0, middle, near, send_rows, False)
    near_half(1)
    halo(near, (1, 2), middle, node_rows, True)
    halos[1] = send_halo(near, (1, 2))
    gather(receiver_line, middle, node_rows, near, recv_rows, True)
    gather(sender_line, middle, node_rows, near, send_rows, True)
    peers = (patches - 1) * coarse_dev
    all_coarse = copy_to(
        everyone.at[pl.ds(0, peers), :], everyone.at[pl.ds(0, peers), :], COARSE, after, h
    )
    all_coarse.wait_recv()
    picked_rows = hot_pick.shape[0]
    picked = table.at[h, pl.ds(first_picked, picked_rows), :]
    table[h, first_picked : first_picked + picked_rows, :] = jnp.dot(
        hot_pick[...], everyone[...], preferred_element_type=jnp.float32
    ).astype(jnp.bfloat16)
    pick_copies = [copy_to(picked, picked, PICKED + n, p, g) for n, g in enumerate((right, left, far))]
    for c in pick_copies:
        c.start()

    far_half(0)
    halo((far,), (3,), 0, middle, False)
    far_half(1)
    halo((far,), (3,), middle, node_rows, True)
    halos[2] = send_halo((far,), (3,))
    gather(receiver_line, 0, node_rows, pair, recv_rows, False)
    for c in halos[1]:
        c.wait_recv()
    for n, g in enumerate((left, right, far)):
        landed = table.at[g, pl.ds(first_picked, picked_rows), :]
        copy_to(landed, landed, PICKED + n, p, right).wait_recv()
    gather(sender_line, node_rows, total_rows, near, send_rows, True)
    for c in halos[0] + halos[2]:
        c.wait_recv()
    gather(sender_line, 0, total_rows, pair, send_rows, False)

    w_out_in.wait()

    def edge_block(i, carry):
        start = pl.multiple_of(i * block, block)
        here = pl.ds(start, block)
        gathered = jnp.concatenate(
            [send_rows[c, here, :] for c in range(columns // LANES)]
            + [recv_rows[c, here, :] for c in range(columns // LANES)],
            axis=1,
        )
        value = pre[here, :] + jnp.dot(
            gathered, w_in[columns:, :], preferred_element_type=jnp.float32
        )
        active = silu(value).astype(jnp.bfloat16)
        output = jnp.dot(active, w_out[...], preferred_element_type=jnp.float32) + b_out_ref[...]
        update = normalize(output, gain_ref[...], shift_ref[...])
        position = start + lax.broadcasted_iota(jnp.int32, (block, 1), 0)
        message = jnp.where(position < count_ref[0], update, 0.0)
        sent[here, :] = message.astype(jnp.bfloat16)
        edges[here, :] = (edges[here, :].astype(jnp.float32) + message).astype(jnp.bfloat16)
        return carry

    lax.fori_loop(0, edge_rows // block, edge_block, 0, unroll=True)

    share_rows = node_rows // shards
    pre_node = pre.at[pl.ds(0, share_rows), :]
    new = send_rows.at[:, pl.ds(0, share_rows), :]
    half = share_rows // 2
    size = half // PIECES

    def sum_at(j):
        node = j * share_rows + lax.broadcasted_iota(jnp.int32, (share_rows, LANES), 0)
        hot = [
            jnp.where(node == jnp.broadcast_to(receivers_ref[k : k + 1, :], node.shape), 1.0, 0.0)
            for k in range(edge_lines)
        ]
        sums[j] = jnp.dot(
            jnp.concatenate([v.astype(jnp.bfloat16) for v in hot], axis=1),
            sent[...],
            preferred_element_type=jnp.float32,
        ).astype(jnp.bfloat16)

    def piece_rows(k):
        return pl.ds(k * size, size)

    def piece_copy(source, target, slot, g):
        return copy_to(source, target, slot, p, g)

    sum_at(far)
    ring = []
    for k in range(PIECES):
        ring.append(piece_copy(sums.at[far, piece_rows(k), :], passed.at[0, piece_rows(k), :], PASS_RIGHT + k, right))
        ring.append(piece_copy(sums.at[far, piece_rows(PIECES + k), :], passed.at[1, piece_rows(k), :], PASS_LEFT + k, left))
    for c in ring:
        c.start()
    sum_at(right)
    plain_right = [
        piece_copy(sums.at[right, piece_rows(PIECES + k), :], plain.at[0, piece_rows(k), :], PLAIN_RIGHT + k, right)
        for k in range(PIECES)
    ]
    for c in plain_right:
        c.start()
    sum_at(left)
    plain_left = [
        piece_copy(sums.at[left, piece_rows(k), :], plain.at[1, piece_rows(k), :], PLAIN_LEFT + k, left)
        for k in range(PIECES)
    ]
    for c in plain_left:
        c.start()

    sum_copies = []
    for k in range(PIECES):
        here = piece_rows(k)
        other = piece_rows(PIECES + k)
        piece_copy(passed.at[0, here, :], passed.at[0, here, :], PASS_RIGHT + k, right).wait_recv()
        sums[right, k * size : (k + 1) * size, :] = (
            sums[right, k * size : (k + 1) * size, :].astype(jnp.float32)
            + passed[0, k * size : (k + 1) * size, :].astype(jnp.float32)
        ).astype(jnp.bfloat16)
        c = piece_copy(sums.at[right, here, :], summed.at[0, here, :], SUM_RIGHT + k, right)
        c.start()
        sum_copies.append(c)
        piece_copy(passed.at[1, here, :], passed.at[1, here, :], PASS_LEFT + k, left).wait_recv()
        sums[left, half + k * size : half + (k + 1) * size, :] = (
            sums[left, half + k * size : half + (k + 1) * size, :].astype(jnp.float32)
            + passed[1, k * size : (k + 1) * size, :].astype(jnp.float32)
        ).astype(jnp.bfloat16)
        c = piece_copy(sums.at[left, other, :], summed.at[1, here, :], SUM_LEFT + k, left)
        c.start()
        sum_copies.append(c)

    sum_at(h)
    w_node_in_in.wait()
    w_node_out_in.wait()

    def own_rows(first, count):
        there = pl.ds(pl.multiple_of(h * share_rows + first, count), count)
        return jnp.concatenate([table[c, there, :] for c in range(columns // LANES)], axis=1)

    pre_node[...] = (
        jnp.dot(
            own_rows(0, share_rows), w_node_in[:columns, :], preferred_element_type=jnp.float32
        )
        + b_node_in_ref[...]
    )

    new_copies = []
    home = []
    for k in range(PIECES):
        here = piece_rows(k)
        spans = ((k * size, 0), (half + k * size, 1))
        piece_copy(summed.at[0, here, :], summed.at[0, here, :], SUM_RIGHT + k, right).wait_recv()
        piece_copy(summed.at[1, here, :], summed.at[1, here, :], SUM_LEFT + k, left).wait_recv()
        piece_copy(plain.at[0, here, :], plain.at[0, here, :], PLAIN_RIGHT + k, right).wait_recv()
        piece_copy(plain.at[1, here, :], plain.at[1, here, :], PLAIN_LEFT + k, left).wait_recv()
        gathered = jnp.concatenate(
            [
                (
                    sums[h, first : first + size, :].astype(jnp.float32)
                    + summed[side, k * size : (k + 1) * size, :].astype(jnp.float32)
                    + plain[1 - side, k * size : (k + 1) * size, :].astype(jnp.float32)
                ).astype(jnp.bfloat16)
                for first, side in spans
            ],
            axis=0,
        )
        value = jnp.concatenate([pre_node[first : first + size, :] for first, side in spans], axis=0)
        value = value + jnp.dot(
            gathered, w_node_in[columns:, :], preferred_element_type=jnp.float32
        )
        active = silu(value).astype(jnp.bfloat16)
        output = jnp.dot(active, w_node_out[...], preferred_element_type=jnp.float32) + b_node_out_ref[...]
        update = normalize(output, node_gain_ref[...], node_shift_ref[...])
        old = jnp.concatenate([own_rows(first, size) for first, side in spans], axis=0)
        result = (old.astype(jnp.float32) + update).astype(jnp.bfloat16)
        for c in range(columns // LANES):
            for n, (first, side) in enumerate(spans):
                new[c, first : first + size, :] = result[
                    n * size : (n + 1) * size, c * LANES : (c + 1) * LANES
                ]
        for n, (first, side) in enumerate(spans):
            there = pl.ds(pl.multiple_of(h * share_rows + first, size), size)
            for m, g in enumerate((far, right, left)):
                c = piece_copy(
                    new.at[g, pl.ds(first, size), :],
                    nodes_out_ref.at[there, :],
                    NEW + (k * 2 + n) * 3 + m,
                    g,
                )
                c.start()
                new_copies.append(c)
    share_there = pl.ds(pl.multiple_of(h * share_rows, share_rows), share_rows)
    nodes_out_ref[share_there, :] = new[h]

    for c in to_right + to_left + relay_right + relay_left + pick_copies:
        c.wait_send()
    for c in halos[0] + halos[1] + halos[2]:
        c.wait_send()
    all_coarse.wait_send()
    for c in ring + plain_right + plain_left + sum_copies + new_copies:
        c.wait_send()
    for k in range(PIECES):
        for n, first in enumerate((k * size, half + k * size)):
            for m, g in enumerate((far, left, right)):
                there = pl.ds(pl.multiple_of(g * share_rows + first, size), size)
                landed = nodes_out_ref.at[there, :]
                piece_copy(landed, landed, NEW + (k * 2 + n) * 3 + m, right).wait_recv()


def layer_stage(
    nodes,
    edges,
    senders,
    receivers,
    halo_rows,
    coarse_rows,
    edge_count,
    w_edge_in,
    b_edge_in,
    w_edge_out,
    b_edge_out,
    edge_gain,
    edge_shift,
    w_node_in,
    b_node_in,
    w_node_out,
    b_node_out,
    node_gain,
    node_shift,
):
    edge_rows, columns = edges.shape
    node_rows = nodes.shape[0]
    border = halo_rows.shape[2]
    picked = coarse_rows.shape[1] * coarse_rows.shape[2]
    total = node_rows + 2 * border + picked
    shards = lax.axis_size("hidden")
    patches = lax.axis_size("patch")
    share_rows = node_rows // shards
    rounds = (patches // 2 - 1).bit_length()
    vmem = pl.BlockSpec(memory_space=pltpu.VMEM)
    smem = pl.BlockSpec(memory_space=pltpu.SMEM)
    far_away = pl.BlockSpec(memory_space=pl.ANY)
    bf16 = jnp.bfloat16
    parts = columns // LANES
    network = [far_away, vmem, far_away, vmem, vmem, vmem]

    def row(v):
        return v.reshape(1, -1)

    return pl.pallas_call(
        lambda *refs: layer_kernel(COARSE_DEV, *refs),
        out_shape=(
            pltpu.VMEM(nodes.shape, bf16),
            pltpu.VMEM((edge_rows, columns), bf16),
        ),
        in_specs=[smem, far_away, far_away, vmem, vmem, vmem, vmem, *network, *network],
        out_specs=(vmem, vmem),
        scratch_shapes=[
            pltpu.VMEM((parts, total, LANES), bf16),
            pltpu.VMEM((parts, 2 * border, LANES), bf16),
            pltpu.VMEM((patches * COARSE_DEV, LANES), bf16),
            pltpu.VMEM((picked, patches * COARSE_DEV), bf16),
            pltpu.VMEM((parts, edge_rows, LANES), bf16),
            pltpu.VMEM((parts, edge_rows, LANES), bf16),
            pltpu.VMEM((edge_rows, columns), jnp.float32),
            pltpu.VMEM((edge_rows, columns), bf16),
            pltpu.VMEM(w_edge_in.shape, bf16),
            pltpu.VMEM(w_edge_out.shape, bf16),
            pltpu.VMEM(w_node_in.shape, bf16),
            pltpu.VMEM(w_node_out.shape, bf16),
            pltpu.VMEM((shards, share_rows, columns), bf16),
            pltpu.VMEM((2, share_rows // 2, columns), bf16),
            pltpu.VMEM((2, share_rows // 2, columns), bf16),
            pltpu.VMEM((2, share_rows // 2, columns), bf16),
            pltpu.SemaphoreType.DMA((SLOTS,)),
            pltpu.SemaphoreType.DMA((SLOTS,)),
            pltpu.SemaphoreType.DMA((LOCALS,)),
            pltpu.SemaphoreType.REGULAR((rounds,)),
        ],
        compiler_params=pltpu.CompilerParams(
            vmem_limit_bytes=64000000, collective_id=0, has_side_effects=True
        ),
    )(
        edge_count,
        nodes,
        edges,
        senders.reshape(-1, LANES),
        receivers.reshape(-1, LANES),
        halo_rows,
        jnp.swapaxes(coarse_rows, 1, 2),
        w_edge_in,
        row(b_edge_in),
        w_edge_out,
        row(b_edge_out),
        row(edge_gain),
        row(edge_shift),
        w_node_in,
        row(b_node_in),
        w_node_out,
        row(b_node_out),
        row(node_gain),
        row(node_shift),
    )


def solution(mesh):
    return jax.shard_map(
        layer_stage,
        mesh=mesh,
        in_specs=(
            P("patch", "hidden"),
            P(("patch", "hidden"), None),
            P(("patch", "hidden")),
            P(("patch", "hidden")),
            P("patch", None, None),
            P("patch", None, None),
            P(("patch", "hidden")),
            *([P()] * 12),
        ),
        out_specs=(P("patch", "hidden"), P(("patch", "hidden"), None)),
        check_vma=False,
    )
```

```python
import jax
import jax.numpy as jnp
from jax import lax
from jax.experimental import pallas as pl
from jax.experimental.pallas import tpu as pltpu
from jax.sharding import PartitionSpec as P

COARSE_DEV = 64
LANES = 128
ROW_BLOCK = 512
LONG_BLOCK = 1024
CHUNKS = 4
MESH = pl.DeviceIdType.MESH


def grid_of(patches):
    return (4, 4, 2) if patches == 32 else (1, 2, patches // 2)


layer_epsilon = 1e-05

TO_RIGHT, TO_LEFT, RELAY_RIGHT, RELAY_LEFT = 0, 4, 8, 10
FORWARD, BACKWARD, COARSE, PICKED = 12, 16, 20, 21
PIECES = 4
PASS_RIGHT, PASS_LEFT = 24, 24 + PIECES
PLAIN_RIGHT, PLAIN_LEFT = 24 + 2 * PIECES, 24 + 3 * PIECES
SUM_RIGHT, SUM_LEFT = 24 + 4 * PIECES, 24 + 5 * PIECES
NEW = 24 + 6 * PIECES
TWIN = NEW + 6 * PIECES
SLOTS = TWIN + 1
L_NODES, L_EDGES, L_IN, L_OUT, L_NODE_IN, L_NODE_OUT, L_RESULT, L_OWN = 0, 1, 2, 3, 4, 5, 6, 7
LOCALS = 8


def normalize(output, norm_gain, norm_shift):
    row_mean = jnp.mean(output, axis=1, keepdims=True)
    centered = output - row_mean
    row_var = jnp.mean(jnp.square(centered), axis=1, keepdims=True)
    return centered * lax.rsqrt(row_var + layer_epsilon) * norm_gain + norm_shift


def silu(v):
    half = 0.5 * v
    return half + half * jnp.tanh(half)


def one_hot(line_of, first, lines, low, high):
    lane = low + lax.broadcasted_iota(jnp.int32, (LANES, LANES), 1)
    rows = []
    for r in range(lines):
        ids = jnp.broadcast_to(line_of(first + r), (LANES, LANES)).T
        rows.append(
            jnp.concatenate(
                [
                    jnp.where(ids == lane + k, 1.0, 0.0).astype(jnp.bfloat16)
                    for k in range(0, high - low, LANES)
                ],
                axis=1,
            )
        )
    return jnp.concatenate(rows, axis=0)


def layer_kernel(
    coarse_dev,
    count_ref,
    nodes_ref,
    edges_ref,
    senders_ref,
    receivers_ref,
    halo_ref,
    coarse_ref,
    w_in_ref,
    b_in_ref,
    w_out_ref,
    b_out_ref,
    gain_ref,
    shift_ref,
    w_node_in_ref,
    b_node_in_ref,
    w_node_out_ref,
    b_node_out_ref,
    node_gain_ref,
    node_shift_ref,
    nodes_out_ref,
    edges_out_ref,
    table,
    outgoing,
    everyone,
    hot_pick,
    send_rows,
    recv_rows,
    pre,
    sent,
    w_in,
    w_out,
    w_node_in,
    w_node_out,
    sums,
    passed,
    plain,
    summed,
    send_sem,
    recv_sem,
    local_sem,
    known_sem,
):
    edges = edges_out_ref
    p, h = lax.axis_index("patch"), lax.axis_index("hidden")
    patches, shards = lax.axis_size("patch"), lax.axis_size("hidden")
    right, left, far = (lax.rem(h + s, shards) for s in (1, shards - 1, 2))
    after, before = lax.rem(p + 1, patches), lax.rem(p + patches - 1, patches)
    node_rows = nodes_ref.shape[0]
    edge_rows, columns = edges_ref.shape
    border = outgoing.shape[1] // 2
    chunk = node_rows // CHUNKS
    block = min(ROW_BLOCK, edge_rows)

    def copy_to(source, target, slot, q, g):
        return pltpu.make_async_remote_copy(
            src_ref=source,
            dst_ref=target,
            send_sem=send_sem.at[slot],
            recv_sem=recv_sem.at[slot],
            device_id={"patch": q, "hidden": g},
            device_id_type=MESH,
        )

    def rows_of(part, k):
        return table.at[part, pl.ds(k * chunk, chunk), :]

    barrier = pltpu.get_barrier_semaphore()

    def signal(sem, q, g):
        pl.semaphore_signal(sem, inc=1, device_id={"patch": q, "hidden": g}, device_id_type=MESH)

    for g in (right, left, far):
        signal(barrier, p, g)
    grid = grid_of(patches)
    nearby, stride, number = [], 1, 0
    for size in reversed(grid):
        spot = lax.rem(lax.div(p, stride), size)
        if size > 1:
            nearby += [(spot > 0, p - stride), (spot < size - 1, p + stride)]
            number = number + jnp.where(spot > 0, 1, 0) + jnp.where(spot < size - 1, 1, 0)
        stride *= size

    def tell(sem):
        for there, q in nearby:
            pl.when(there)(lambda q=q: signal(sem, lax.rem(q + patches, patches), h))

    tell(barrier)

    nodes_in = pltpu.make_async_copy(
        nodes_ref, table.at[h, pl.ds(0, node_rows), :], local_sem.at[L_NODES]
    )
    edges_in = pltpu.make_async_copy(edges_ref, edges, local_sem.at[L_EDGES])
    w_in_in = pltpu.make_async_copy(w_in_ref, w_in, local_sem.at[L_IN])
    w_out_in = pltpu.make_async_copy(w_out_ref, w_out, local_sem.at[L_OUT])
    w_node_in_in = pltpu.make_async_copy(w_node_in_ref, w_node_in, local_sem.at[L_NODE_IN])
    w_node_out_in = pltpu.make_async_copy(w_node_out_ref, w_node_out, local_sem.at[L_NODE_OUT])
    for c in (nodes_in, edges_in, w_in_in, w_out_in, w_node_in_in, w_node_out_in):
        c.start()

    lines = border // LANES

    def halo_line(r):
        side, place = lax.div(r, lines), lax.rem(r, lines)
        both = halo_ref[0, :, pl.ds(pl.multiple_of(place * LANES, LANES), LANES)]
        return jnp.where(side == 0, both[:1], both[1:])

    def loop(count, body):
        lax.fori_loop(0, count, lambda i, carry: (body(i), carry)[1], 0)

    pl.semaphore_wait(barrier, shards - 1 + number)

    rounds = known_sem.shape[0]
    tell(known_sem.at[0])

    def learned(r):
        if r < rounds:
            pl.semaphore_wait(known_sem.at[r], number)
            if r + 1 < rounds:
                tell(known_sem.at[r + 1])

    nodes_in.wait()

    to_right = [copy_to(rows_of(h, k), rows_of(h, k), TO_RIGHT + k, p, right) for k in range(CHUNKS)]
    to_left = [copy_to(rows_of(h, k), rows_of(h, k), TO_LEFT + k, p, left) for k in range(CHUNKS)]
    for a, b in ((0, 1), (1, 0), (2, 3), (3, 2)):
        to_right[a].start()
        to_left[b].start()


    long_block = min(LONG_BLOCK, edge_rows, 2 * border)
    long_lines = long_block // LANES
    border_blocks = 2 * border // long_block
    gather_blocks = edge_rows // long_block

    def side(parts, low, high):
        return jnp.concatenate([table[c, low:high, :] for c in parts], axis=1)

    def halo(parts, names, low, high, add):
        def piece(i):
            here = pl.ds(pl.multiple_of(i * long_block, long_block), long_block)
            result = jnp.dot(
                one_hot(halo_line, i * long_lines, long_lines, low, high),
                side(parts, low, high),
                preferred_element_type=jnp.float32,
            ).astype(jnp.bfloat16)
            for n, name in enumerate(names):
                value = result[:, n * LANES : (n + 1) * LANES]
                outgoing[name, here, :] = outgoing[name, here, :] + value if add else value

        loop(border_blocks, piece)

    def send_halo(parts, names):
        copies = []
        for part, name in zip(parts, names):
            back = copy_to(
                outgoing.at[name, pl.ds(0, border), :],
                table.at[part, pl.ds(node_rows + border, border), :],
                BACKWARD + name,
                before,
                h,
            )
            forth = copy_to(
                outgoing.at[name, pl.ds(border, border), :],
                table.at[part, pl.ds(node_rows, border), :],
                FORWARD + name,
                after,
                h,
            )
            back.start()
            forth.start()
            copies += [back, forth]
        return copies

    halos = {}
    edge_lines = edge_rows // LANES
    middle = node_rows // 2
    halo((h,), (0,), 0, node_rows, False)
    learned(0)

    edges_in.wait()
    w_in_in.wait()

    per_slot = hot_pick.shape[0] // patches
    first_picked = node_rows + 2 * border

    def sender_line(r):
        code = senders_ref[pl.ds(r, 1), :]
        slot = code - first_picked
        moved = lax.rem(slot, per_slot) * patches + lax.div(slot, per_slot)
        return jnp.where(slot >= 0, first_picked + moved, code)

    def self_block(i, carry):
        here = pl.ds(pl.multiple_of(i * block, block), block)
        pre[here, :] = (
            jnp.dot(edges[here, :], w_in[:columns, :], preferred_element_type=jnp.float32)
            + b_in_ref[...]
        )
        return carry

    edge_blocks = edge_rows // block
    lax.fori_loop(0, edge_blocks // 2, self_block, 0)
    learned(1)
    lax.fori_loop(edge_blocks // 2, edge_blocks, self_block, 0)
    learned(2)
    learned(3)

    owner = lax.broadcasted_iota(jnp.int32, (patches, LANES), 0)
    owner = (lax.rem(owner, 2) * (patches // 2) + lax.div(owner, 2)) * coarse_dev
    spot = lax.broadcasted_iota(jnp.int32, (patches, LANES), 1)
    for k in range(per_slot):
        line = coarse_ref[0, k : k + 1, :]
        wanted = jnp.broadcast_to(line, (LANES, patches)).T + owner
        for b in range(hot_pick.shape[1] // LANES):
            hot_pick[k * patches : (k + 1) * patches, b * LANES : (b + 1) * LANES] = jnp.where(
                wanted == spot + b * LANES, 1.0, 0.0
            ).astype(jnp.bfloat16)

    def from_left(k):
        return copy_to(rows_of(left, k), rows_of(left, k), TO_RIGHT + k, p, right)

    def from_right(k):
        return copy_to(rows_of(right, k), rows_of(right, k), TO_LEFT + k, p, left)

    relay_right = [copy_to(rows_of(left, 2 * k), rows_of(left, 2 * k), RELAY_RIGHT + k, p, right) for k in (0, 1)]
    relay_left = [copy_to(rows_of(right, 2 * k + 1), rows_of(right, 2 * k + 1), RELAY_LEFT + k, p, left) for k in (0, 1)]

    def near_half(k):
        for c in (2 * k, 2 * k + 1):
            from_left(c).wait_recv()
            from_right(c).wait_recv()
        relay_right[k].start()
        relay_left[k].start()

    def far_half(k):
        copy_to(rows_of(far, 2 * k), rows_of(far, 2 * k), RELAY_RIGHT + k, p, right).wait_recv()
        copy_to(rows_of(far, 2 * k + 1), rows_of(far, 2 * k + 1), RELAY_LEFT + k, p, left).wait_recv()

    def gather(line_of, low, high, parts, into, add):
        def piece(i):
            here = pl.ds(pl.multiple_of(i * long_block, long_block), long_block)
            result = jnp.dot(
                one_hot(line_of, i * long_lines, long_lines, low, high),
                side(parts, low, high),
                preferred_element_type=jnp.float32,
            ).astype(jnp.bfloat16)
            for n, c in enumerate(parts):
                value = result[:, n * LANES : (n + 1) * LANES]
                into[c, here, :] = into[c, here, :] + value if add else value

        loop(gather_blocks, piece)

    def receiver_line(r):
        return receivers_ref[pl.ds(r, 1), :]

    near, pair = (left, right), (h, far)
    total_rows = table.shape[1]
    learned(4)
    learned(5)
    halos[0] = send_halo((h,), (0,))
    chips = patches // 2
    chip, core = lax.div(p, 2), lax.rem(p, 2)
    mine_first = pl.multiple_of((core * chips + chip) * coarse_dev, coarse_dev)
    slot_rows = pl.ds(mine_first, coarse_dev)
    own_coarse = table.at[h, pl.ds(0, coarse_dev), :]

    def share(j, carry):
        copy_to(own_coarse, everyone.at[slot_rows, :], COARSE, lax.rem(p + 2 * j, patches), h).start()
        return carry

    lax.fori_loop(1, chips, share, 0)
    everyone[slot_rows, :] = own_coarse[...]
    near_half(0)
    halo(near, (1, 2), 0, middle, False)
    gather(receiver_line, 0, middle, near, recv_rows, False)
    gather(sender_line, 0, middle, near, send_rows, False)
    near_half(1)
    halo(near, (1, 2), middle, node_rows, True)
    halos[1] = send_halo(near, (1, 2))
    gather(receiver_line, middle, node_rows, near, recv_rows, True)
    gather(sender_line, middle, node_rows, near, send_rows, True)
    peers = (chips - 1) * coarse_dev
    all_coarse = copy_to(
        everyone.at[pl.ds(0, peers), :], everyone.at[pl.ds(0, peers), :], COARSE, after, h
    )
    all_coarse.wait_recv()
    group = chips * coarse_dev
    same_core = everyone.at[pl.ds(pl.multiple_of(core * group, group), group), :]
    to_twin = copy_to(same_core, same_core, TWIN, p + 1 - 2 * core, h)
    to_twin.start()
    far_half(0)
    halo((far,), (3,), 0, middle, False)
    far_half(1)
    halo((far,), (3,), middle, node_rows, True)
    halos[2] = send_halo((far,), (3,))
    copy_to(same_core, same_core, TWIN, p + 1 - 2 * core, h).wait_recv()
    picked_rows = hot_pick.shape[0]
    picked = table.at[h, pl.ds(first_picked, picked_rows), :]
    table[h, first_picked : first_picked + picked_rows, :] = jnp.dot(
        hot_pick[...], everyone[...], preferred_element_type=jnp.float32
    ).astype(jnp.bfloat16)
    pick_copies = [copy_to(picked, picked, PICKED + n, p, g) for n, g in enumerate((right, left, far))]
    for c in pick_copies:
        c.start()
    gather(receiver_line, 0, node_rows, pair, recv_rows, False)
    gather(sender_line, 0, node_rows, pair, send_rows, False)
    for c in halos[1]:
        c.wait_recv()
    for n, g in enumerate((left, right, far)):
        landed = table.at[g, pl.ds(first_picked, picked_rows), :]
        copy_to(landed, landed, PICKED + n, p, right).wait_recv()
    gather(sender_line, node_rows, total_rows, near, send_rows, True)
    for c in halos[0] + halos[2]:
        c.wait_recv()
    gather(sender_line, node_rows, total_rows, pair, send_rows, True)

    w_out_in.wait()

    def edge_block(i, carry):
        start = pl.multiple_of(i * block, block)
        here = pl.ds(start, block)
        parts = range(columns // LANES)
        gathered = jnp.concatenate(
            [send_rows[c, here, :] for c in parts]
            + [recv_rows[c, here, :] for c in parts],
            axis=1,
        )
        value = pre[here, :] + jnp.dot(
            gathered, w_in[columns:, :], preferred_element_type=jnp.float32
        )
        active = silu(value).astype(jnp.bfloat16)
        output = jnp.dot(active, w_out[...], preferred_element_type=jnp.float32) + b_out_ref[...]
        update = normalize(output, gain_ref[...], shift_ref[...])
        position = start + lax.broadcasted_iota(jnp.int32, (block, 1), 0)
        message = jnp.where(position < count_ref[0], update, 0.0)
        sent[here, :] = message.astype(jnp.bfloat16)
        edges[here, :] = (edges[here, :].astype(jnp.float32) + message).astype(jnp.bfloat16)
        return carry

    lax.fori_loop(0, edge_rows // block, edge_block, 0, unroll=True)

    share_rows = node_rows // shards
    pre_node = pre.at[pl.ds(0, share_rows), :]
    new = send_rows.at[:, pl.ds(0, share_rows), :]
    half = share_rows // 2
    size = half // PIECES

    def sum_at(j):
        node = j * share_rows + lax.broadcasted_iota(jnp.int32, (share_rows, LANES), 0)
        hot = [
            jnp.where(node == jnp.broadcast_to(receivers_ref[k : k + 1, :], node.shape), 1.0, 0.0)
            for k in range(edge_lines)
        ]
        sums[j] = jnp.dot(
            jnp.concatenate([v.astype(jnp.bfloat16) for v in hot], axis=1),
            sent[...],
            preferred_element_type=jnp.float32,
        ).astype(jnp.bfloat16)

    def piece_rows(k):
        return pl.ds(k * size, size)

    def piece_copy(source, target, slot, g):
        return copy_to(source, target, slot, p, g)

    sum_at(far)
    ring = []
    for k in range(PIECES):
        ring.append(piece_copy(sums.at[far, piece_rows(k), :], passed.at[0, piece_rows(k), :], PASS_RIGHT + k, right))
        ring.append(piece_copy(sums.at[far, piece_rows(PIECES + k), :], passed.at[1, piece_rows(k), :], PASS_LEFT + k, left))
    for c in ring:
        c.start()
    sum_at(right)
    plain_right = [
        piece_copy(sums.at[right, piece_rows(PIECES + k), :], plain.at[0, piece_rows(k), :], PLAIN_RIGHT + k, right)
        for k in range(PIECES)
    ]
    for c in plain_right:
        c.start()
    sum_at(left)
    plain_left = [
        piece_copy(sums.at[left, piece_rows(k), :], plain.at[1, piece_rows(k), :], PLAIN_LEFT + k, left)
        for k in range(PIECES)
    ]
    for c in plain_left:
        c.start()

    sum_copies = []
    for k in range(PIECES):
        here = piece_rows(k)
        other = piece_rows(PIECES + k)
        piece_copy(passed.at[0, here, :], passed.at[0, here, :], PASS_RIGHT + k, right).wait_recv()
        sums[right, k * size : (k + 1) * size, :] = (
            sums[right, k * size : (k + 1) * size, :].astype(jnp.float32)
            + passed[0, k * size : (k + 1) * size, :].astype(jnp.float32)
        ).astype(jnp.bfloat16)
        c = piece_copy(sums.at[right, here, :], summed.at[0, here, :], SUM_RIGHT + k, right)
        c.start()
        sum_copies.append(c)
        piece_copy(passed.at[1, here, :], passed.at[1, here, :], PASS_LEFT + k, left).wait_recv()
        sums[left, half + k * size : half + (k + 1) * size, :] = (
            sums[left, half + k * size : half + (k + 1) * size, :].astype(jnp.float32)
            + passed[1, k * size : (k + 1) * size, :].astype(jnp.float32)
        ).astype(jnp.bfloat16)
        c = piece_copy(sums.at[left, other, :], summed.at[1, here, :], SUM_LEFT + k, left)
        c.start()
        sum_copies.append(c)

    sum_at(h)
    w_node_in_in.wait()
    w_node_out_in.wait()

    def own_rows(first, count):
        there = pl.ds(pl.multiple_of(h * share_rows + first, count), count)
        return jnp.concatenate([table[c, there, :] for c in range(columns // LANES)], axis=1)

    pre_node[...] = (
        jnp.dot(
            own_rows(0, share_rows), w_node_in[:columns, :], preferred_element_type=jnp.float32
        )
        + b_node_in_ref[...]
    )

    new_copies = []
    home = []
    for k in range(PIECES):
        here = piece_rows(k)
        spans = ((k * size, 0), (half + k * size, 1))
        piece_copy(summed.at[0, here, :], summed.at[0, here, :], SUM_RIGHT + k, right).wait_recv()
        piece_copy(summed.at[1, here, :], summed.at[1, here, :], SUM_LEFT + k, left).wait_recv()
        piece_copy(plain.at[0, here, :], plain.at[0, here, :], PLAIN_RIGHT + k, right).wait_recv()
        piece_copy(plain.at[1, here, :], plain.at[1, here, :], PLAIN_LEFT + k, left).wait_recv()
        gathered = jnp.concatenate(
            [
                (
                    sums[h, first : first + size, :].astype(jnp.float32)
                    + summed[side, k * size : (k + 1) * size, :].astype(jnp.float32)
                    + plain[1 - side, k * size : (k + 1) * size, :].astype(jnp.float32)
                ).astype(jnp.bfloat16)
                for first, side in spans
            ],
            axis=0,
        )
        value = jnp.concatenate([pre_node[first : first + size, :] for first, side in spans], axis=0)
        value = value + jnp.dot(
            gathered, w_node_in[columns:, :], preferred_element_type=jnp.float32
        )
        active = silu(value).astype(jnp.bfloat16)
        output = jnp.dot(active, w_node_out[...], preferred_element_type=jnp.float32) + b_node_out_ref[...]
        update = normalize(output, node_gain_ref[...], node_shift_ref[...])
        old = jnp.concatenate([own_rows(first, size) for first, side in spans], axis=0)
        result = (old.astype(jnp.float32) + update).astype(jnp.bfloat16)
        for c in range(columns // LANES):
            for n, (first, side) in enumerate(spans):
                new[c, first : first + size, :] = result[
                    n * size : (n + 1) * size, c * LANES : (c + 1) * LANES
                ]
        for n, (first, side) in enumerate(spans):
            there = pl.ds(pl.multiple_of(h * share_rows + first, size), size)
            for m, g in enumerate((far, right, left)):
                c = piece_copy(
                    new.at[g, pl.ds(first, size), :],
                    nodes_out_ref.at[there, :],
                    NEW + (k * 2 + n) * 3 + m,
                    g,
                )
                c.start()
                new_copies.append(c)
    share_there = pl.ds(pl.multiple_of(h * share_rows, share_rows), share_rows)
    nodes_out_ref[share_there, :] = new[h]

    for c in to_right + to_left + relay_right + relay_left + pick_copies:
        c.wait_send()
    for c in halos[0] + halos[1] + halos[2]:
        c.wait_send()
    all_coarse.wait_send()
    to_twin.wait_send()
    for c in ring + plain_right + plain_left + sum_copies + new_copies:
        c.wait_send()
    for k in range(PIECES):
        for n, first in enumerate((k * size, half + k * size)):
            for m, g in enumerate((far, left, right)):
                there = pl.ds(pl.multiple_of(g * share_rows + first, size), size)
                landed = nodes_out_ref.at[there, :]
                piece_copy(landed, landed, NEW + (k * 2 + n) * 3 + m, right).wait_recv()


def layer_stage(
    nodes,
    edges,
    senders,
    receivers,
    halo_rows,
    coarse_rows,
    edge_count,
    w_edge_in,
    b_edge_in,
    w_edge_out,
    b_edge_out,
    edge_gain,
    edge_shift,
    w_node_in,
    b_node_in,
    w_node_out,
    b_node_out,
    node_gain,
    node_shift,
):
    edge_rows, columns = edges.shape
    node_rows = nodes.shape[0]
    border = halo_rows.shape[2]
    picked = coarse_rows.shape[1] * coarse_rows.shape[2]
    total = node_rows + 2 * border + picked
    shards = lax.axis_size("hidden")
    patches = lax.axis_size("patch")
    share_rows = node_rows // shards
    rounds = sum(grid_of(patches)) - 4
    vmem = pl.BlockSpec(memory_space=pltpu.VMEM)
    smem = pl.BlockSpec(memory_space=pltpu.SMEM)
    far_away = pl.BlockSpec(memory_space=pl.ANY)
    bf16 = jnp.bfloat16
    parts = columns // LANES
    network = [far_away, vmem, far_away, vmem, vmem, vmem]

    def row(v):
        return v.reshape(1, -1)

    return pl.pallas_call(
        lambda *refs: layer_kernel(COARSE_DEV, *refs),
        out_shape=(
            pltpu.VMEM(nodes.shape, bf16),
            pltpu.VMEM((edge_rows, columns), bf16),
        ),
        in_specs=[smem, far_away, far_away, vmem, vmem, vmem, vmem, *network, *network],
        out_specs=(vmem, vmem),
        scratch_shapes=[
            pltpu.VMEM((parts, total, LANES), bf16),
            pltpu.VMEM((parts, 2 * border, LANES), bf16),
            pltpu.VMEM((patches * COARSE_DEV, LANES), bf16),
            pltpu.VMEM((picked, patches * COARSE_DEV), bf16),
            pltpu.VMEM((parts, edge_rows, LANES), bf16),
            pltpu.VMEM((parts, edge_rows, LANES), bf16),
            pltpu.VMEM((edge_rows, columns), jnp.float32),
            pltpu.VMEM((edge_rows, columns), bf16),
            pltpu.VMEM(w_edge_in.shape, bf16),
            pltpu.VMEM(w_edge_out.shape, bf16),
            pltpu.VMEM(w_node_in.shape, bf16),
            pltpu.VMEM(w_node_out.shape, bf16),
            pltpu.VMEM((shards, share_rows, columns), bf16),
            pltpu.VMEM((2, share_rows // 2, columns), bf16),
            pltpu.VMEM((2, share_rows // 2, columns), bf16),
            pltpu.VMEM((2, share_rows // 2, columns), bf16),
            pltpu.SemaphoreType.DMA((SLOTS,)),
            pltpu.SemaphoreType.DMA((SLOTS,)),
            pltpu.SemaphoreType.DMA((LOCALS,)),
            pltpu.SemaphoreType.REGULAR((rounds,)),
        ],
        compiler_params=pltpu.CompilerParams(
            vmem_limit_bytes=64000000, collective_id=0, has_side_effects=True
        ),
    )(
        edge_count,
        nodes,
        edges,
        senders.reshape(-1, LANES),
        receivers.reshape(-1, LANES),
        halo_rows,
        jnp.swapaxes(coarse_rows, 1, 2),
        w_edge_in,
        row(b_edge_in),
        w_edge_out,
        row(b_edge_out),
        row(edge_gain),
        row(edge_shift),
        w_node_in,
        row(b_node_in),
        w_node_out,
        row(b_node_out),
        row(node_gain),
        row(node_shift),
    )


def solution(mesh):
    return jax.shard_map(
        layer_stage,
        mesh=mesh,
        in_specs=(
            P("patch", "hidden"),
            P(("patch", "hidden"), None),
            P(("patch", "hidden")),
            P(("patch", "hidden")),
            P("patch", None, None),
            P("patch", None, None),
            P(("patch", "hidden")),
            *([P()] * 12),
        ),
        out_specs=(P("patch", "hidden"), P(("patch", "hidden"), None)),
        check_vma=False,
    )
```

```python
import jax
import jax.numpy as jnp
from jax import lax
from jax.experimental import pallas as pl
from jax.experimental.pallas import tpu as pltpu
from jax.sharding import PartitionSpec as P

COARSE_DEV = 64
LANES = 128
ROW_BLOCK = 512
LONG_BLOCK = 1024
CHUNKS = 4
MESH = pl.DeviceIdType.MESH


def grid_of(patches):
    return (4, 4, 2) if patches == 32 else (1, 2, patches // 2)


layer_epsilon = 1e-05

TO_RIGHT, TO_LEFT, RELAY_RIGHT, RELAY_LEFT = 0, 4, 8, 10
FORWARD, BACKWARD, COARSE, PICKED = 12, 16, 20, 21
PIECES = 4
PASS_RIGHT, PASS_LEFT = 24, 24 + PIECES
PLAIN_RIGHT, PLAIN_LEFT = 24 + 2 * PIECES, 24 + 3 * PIECES
SUM_RIGHT, SUM_LEFT = 24 + 4 * PIECES, 24 + 5 * PIECES
NEW = 24 + 6 * PIECES
TWIN = NEW + 6 * PIECES
SLOTS = TWIN + 1
L_NODES, L_EDGES, L_IN, L_OUT, L_NODE_IN, L_NODE_OUT, L_RESULT, L_OWN = 0, 1, 2, 3, 4, 5, 6, 7
LOCALS = 8


def normalize(output, norm_gain, norm_shift):
    row_mean = jnp.mean(output, axis=1, keepdims=True)
    centered = output - row_mean
    row_var = jnp.mean(jnp.square(centered), axis=1, keepdims=True)
    return centered * lax.rsqrt(row_var + layer_epsilon) * norm_gain + norm_shift


def silu(v):
    half = 0.5 * v
    return half + half * jnp.tanh(half)


def one_hot(line_of, first, lines, low, high):
    lane = low + lax.broadcasted_iota(jnp.int32, (LANES, LANES), 1)
    rows = []
    for r in range(lines):
        ids = jnp.broadcast_to(line_of(first + r), (LANES, LANES)).T
        rows.append(
            jnp.concatenate(
                [
                    jnp.where(ids == lane + k, 1.0, 0.0).astype(jnp.bfloat16)
                    for k in range(0, high - low, LANES)
                ],
                axis=1,
            )
        )
    return jnp.concatenate(rows, axis=0)


def layer_kernel(
    coarse_dev,
    count_ref,
    nodes_ref,
    edges_ref,
    senders_ref,
    receivers_ref,
    halo_ref,
    coarse_ref,
    w_in_ref,
    b_in_ref,
    w_out_ref,
    b_out_ref,
    gain_ref,
    shift_ref,
    w_node_in_ref,
    b_node_in_ref,
    w_node_out_ref,
    b_node_out_ref,
    node_gain_ref,
    node_shift_ref,
    nodes_out_ref,
    edges_out_ref,
    table,
    outgoing,
    everyone,
    hot_pick,
    send_rows,
    recv_rows,
    pre,
    sent,
    w_in,
    w_out,
    w_node_in,
    w_node_out,
    sums,
    passed,
    plain,
    summed,
    send_sem,
    recv_sem,
    local_sem,
    known_sem,
):
    edges = edges_out_ref
    p, h = lax.axis_index("patch"), lax.axis_index("hidden")
    patches, shards = lax.axis_size("patch"), lax.axis_size("hidden")
    right, left, far = (lax.rem(h + s, shards) for s in (1, shards - 1, 2))
    after, before = lax.rem(p + 1, patches), lax.rem(p + patches - 1, patches)
    node_rows = nodes_ref.shape[0]
    edge_rows, columns = edges_ref.shape
    border = outgoing.shape[1] // 2
    chunk = node_rows // CHUNKS
    block = min(ROW_BLOCK, edge_rows)

    def copy_to(source, target, slot, q, g):
        return pltpu.make_async_remote_copy(
            src_ref=source,
            dst_ref=target,
            send_sem=send_sem.at[slot],
            recv_sem=recv_sem.at[slot],
            device_id={"patch": q, "hidden": g},
            device_id_type=MESH,
        )

    def rows_of(part, k):
        return table.at[part, pl.ds(k * chunk, chunk), :]

    barrier = pltpu.get_barrier_semaphore()

    def signal(sem, q, g):
        pl.semaphore_signal(sem, inc=1, device_id={"patch": q, "hidden": g}, device_id_type=MESH)

    for g in (right, left, far):
        signal(barrier, p, g)
    grid = grid_of(patches)
    nearby, stride, number = [], 1, 0
    for size in reversed(grid):
        spot = lax.rem(lax.div(p, stride), size)
        if size > 1:
            nearby += [(spot > 0, p - stride), (spot < size - 1, p + stride)]
            number = number + jnp.where(spot > 0, 1, 0) + jnp.where(spot < size - 1, 1, 0)
        stride *= size

    def tell(sem):
        for there, q in nearby:
            pl.when(there)(lambda q=q: signal(sem, lax.rem(q + patches, patches), h))

    tell(barrier)

    nodes_in = pltpu.make_async_copy(
        nodes_ref, table.at[h, pl.ds(0, node_rows), :], local_sem.at[L_NODES]
    )
    edges_in = pltpu.make_async_copy(edges_ref, edges, local_sem.at[L_EDGES])
    w_in_in = pltpu.make_async_copy(w_in_ref, w_in, local_sem.at[L_IN])
    w_out_in = pltpu.make_async_copy(w_out_ref, w_out, local_sem.at[L_OUT])
    w_node_in_in = pltpu.make_async_copy(w_node_in_ref, w_node_in, local_sem.at[L_NODE_IN])
    w_node_out_in = pltpu.make_async_copy(w_node_out_ref, w_node_out, local_sem.at[L_NODE_OUT])
    for c in (nodes_in, edges_in, w_in_in, w_out_in, w_node_in_in, w_node_out_in):
        c.start()

    lines = border // LANES

    def halo_line(r):
        side, place = lax.div(r, lines), lax.rem(r, lines)
        both = halo_ref[0, :, pl.ds(pl.multiple_of(place * LANES, LANES), LANES)]
        return jnp.where(side == 0, both[:1], both[1:])

    def loop(count, body):
        lax.fori_loop(0, count, lambda i, carry: (body(i), carry)[1], 0)

    pl.semaphore_wait(barrier, shards - 1 + number)

    rounds = known_sem.shape[0]
    tell(known_sem.at[0])

    def learned(r):
        if r < rounds:
            pl.semaphore_wait(known_sem.at[r], number)
            if r + 1 < rounds:
                tell(known_sem.at[r + 1])

    nodes_in.wait()

    to_right = [copy_to(rows_of(h, k), rows_of(h, k), TO_RIGHT + k, p, right) for k in range(CHUNKS)]
    to_left = [copy_to(rows_of(h, k), rows_of(h, k), TO_LEFT + k, p, left) for k in range(CHUNKS)]
    for a, b in ((0, 1), (1, 0), (2, 3), (3, 2)):
        to_right[a].start()
        to_left[b].start()


    long_block = min(LONG_BLOCK, edge_rows, 2 * border)
    long_lines = long_block // LANES
    border_blocks = 2 * border // long_block
    gather_blocks = edge_rows // long_block

    def side(parts, low, high):
        return jnp.concatenate([table[c, low:high, :] for c in parts], axis=1)

    def halo(parts, names, low, high, add):
        def piece(i):
            here = pl.ds(pl.multiple_of(i * long_block, long_block), long_block)
            result = jnp.dot(
                one_hot(halo_line, i * long_lines, long_lines, low, high),
                side(parts, low, high),
                preferred_element_type=jnp.float32,
            ).astype(jnp.bfloat16)
            for n, name in enumerate(names):
                value = result[:, n * LANES : (n + 1) * LANES]
                outgoing[name, here, :] = outgoing[name, here, :] + value if add else value

        loop(border_blocks, piece)

    def send_halo(parts, names):
        copies = []
        for part, name in zip(parts, names):
            back = copy_to(
                outgoing.at[name, pl.ds(0, border), :],
                table.at[part, pl.ds(node_rows + border, border), :],
                BACKWARD + name,
                before,
                h,
            )
            forth = copy_to(
                outgoing.at[name, pl.ds(border, border), :],
                table.at[part, pl.ds(node_rows, border), :],
                FORWARD + name,
                after,
                h,
            )
            back.start()
            forth.start()
            copies += [back, forth]
        return copies

    halos = {}
    edge_lines = edge_rows // LANES
    middle = node_rows // 2
    halo((h,), (0,), 0, node_rows, False)
    learned(0)

    edges_in.wait()
    w_in_in.wait()

    per_slot = hot_pick.shape[0] // patches
    first_picked = node_rows + 2 * border

    def sender_line(r):
        code = senders_ref[pl.ds(r, 1), :]
        slot = code - first_picked
        moved = lax.rem(slot, per_slot) * patches + lax.div(slot, per_slot)
        return jnp.where(slot >= 0, first_picked + moved, code)

    def self_block(i, carry):
        here = pl.ds(pl.multiple_of(i * block, block), block)
        pre[here, :] = (
            jnp.dot(edges[here, :], w_in[:columns, :], preferred_element_type=jnp.float32)
            + b_in_ref[...]
        )
        return carry

    edge_blocks = edge_rows // block
    lax.fori_loop(0, edge_blocks // 2, self_block, 0)
    learned(1)
    lax.fori_loop(edge_blocks // 2, edge_blocks, self_block, 0)
    learned(2)
    learned(3)

    owner = lax.broadcasted_iota(jnp.int32, (patches, LANES), 0)
    owner = (lax.rem(owner, 2) * (patches // 2) + lax.div(owner, 2)) * coarse_dev
    spot = lax.broadcasted_iota(jnp.int32, (patches, LANES), 1)
    for k in range(per_slot):
        line = coarse_ref[0, k : k + 1, :]
        wanted = jnp.broadcast_to(line, (LANES, patches)).T + owner
        for b in range(hot_pick.shape[1] // LANES):
            hot_pick[k * patches : (k + 1) * patches, b * LANES : (b + 1) * LANES] = jnp.where(
                wanted == spot + b * LANES, 1.0, 0.0
            ).astype(jnp.bfloat16)

    def from_left(k):
        return copy_to(rows_of(left, k), rows_of(left, k), TO_RIGHT + k, p, right)

    def from_right(k):
        return copy_to(rows_of(right, k), rows_of(right, k), TO_LEFT + k, p, left)

    relay_right = [copy_to(rows_of(left, 2 * k), rows_of(left, 2 * k), RELAY_RIGHT + k, p, right) for k in (0, 1)]
    relay_left = [copy_to(rows_of(right, 2 * k + 1), rows_of(right, 2 * k + 1), RELAY_LEFT + k, p, left) for k in (0, 1)]

    def near_half(k):
        for c in (2 * k, 2 * k + 1):
            from_left(c).wait_recv()
            from_right(c).wait_recv()
        relay_right[k].start()
        relay_left[k].start()

    def far_half(k):
        copy_to(rows_of(far, 2 * k), rows_of(far, 2 * k), RELAY_RIGHT + k, p, right).wait_recv()
        copy_to(rows_of(far, 2 * k + 1), rows_of(far, 2 * k + 1), RELAY_LEFT + k, p, left).wait_recv()

    def gather(line_of, low, high, parts, into, add):
        def piece(i):
            here = pl.ds(pl.multiple_of(i * long_block, long_block), long_block)
            result = jnp.dot(
                one_hot(line_of, i * long_lines, long_lines, low, high),
                side(parts, low, high),
                preferred_element_type=jnp.float32,
            ).astype(jnp.bfloat16)
            for n, c in enumerate(parts):
                value = result[:, n * LANES : (n + 1) * LANES]
                into[c, here, :] = into[c, here, :] + value if add else value

        loop(gather_blocks, piece)

    def receiver_line(r):
        return receivers_ref[pl.ds(r, 1), :]

    near, pair = (left, right), (h, far)
    total_rows = table.shape[1]
    near_half(0)
    halo(near, (1, 2), 0, middle, False)
    learned(4)
    gather(receiver_line, 0, middle, near, recv_rows, False)
    learned(5)
    halos[0] = send_halo((h,), (0,))
    chips = patches // 2
    chip, core = lax.div(p, 2), lax.rem(p, 2)
    mine_first = pl.multiple_of((core * chips + chip) * coarse_dev, coarse_dev)
    slot_rows = pl.ds(mine_first, coarse_dev)
    own_coarse = table.at[h, pl.ds(0, coarse_dev), :]

    def share(j, carry):
        copy_to(own_coarse, everyone.at[slot_rows, :], COARSE, lax.rem(p + 2 * j, patches), h).start()
        return carry

    lax.fori_loop(1, chips, share, 0)
    everyone[slot_rows, :] = own_coarse[...]
    gather(sender_line, 0, middle, near, send_rows, False)
    near_half(1)
    halo(near, (1, 2), middle, node_rows, True)
    halos[1] = send_halo(near, (1, 2))
    gather(receiver_line, middle, node_rows, near, recv_rows, True)
    gather(sender_line, middle, node_rows, near, send_rows, True)
    far_half(0)
    halo((far,), (3,), 0, middle, False)
    peers = (chips - 1) * coarse_dev
    all_coarse = copy_to(
        everyone.at[pl.ds(0, peers), :], everyone.at[pl.ds(0, peers), :], COARSE, after, h
    )
    all_coarse.wait_recv()
    group = chips * coarse_dev
    same_core = everyone.at[pl.ds(pl.multiple_of(core * group, group), group), :]
    to_twin = copy_to(same_core, same_core, TWIN, p + 1 - 2 * core, h)
    to_twin.start()
    far_half(1)
    halo((far,), (3,), middle, node_rows, True)
    halos[2] = send_halo((far,), (3,))
    copy_to(same_core, same_core, TWIN, p + 1 - 2 * core, h).wait_recv()
    picked_rows = hot_pick.shape[0]
    picked = table.at[h, pl.ds(first_picked, picked_rows), :]
    table[h, first_picked : first_picked + picked_rows, :] = jnp.dot(
        hot_pick[...], everyone[...], preferred_element_type=jnp.float32
    ).astype(jnp.bfloat16)
    pick_copies = [copy_to(picked, picked, PICKED + n, p, g) for n, g in enumerate((right, left, far))]
    for c in pick_copies:
        c.start()
    gather(receiver_line, 0, node_rows, pair, recv_rows, False)
    gather(sender_line, 0, node_rows, pair, send_rows, False)
    for c in halos[1]:
        c.wait_recv()
    for n, g in enumerate((left, right, far)):
        landed = table.at[g, pl.ds(first_picked, picked_rows), :]
        copy_to(landed, landed, PICKED + n, p, right).wait_recv()
    gather(sender_line, node_rows, total_rows, near, send_rows, True)
    for c in halos[0] + halos[2]:
        c.wait_recv()
    gather(sender_line, node_rows, total_rows, pair, send_rows, True)

    w_out_in.wait()

    def edge_block(i, carry):
        start = pl.multiple_of(i * block, block)
        here = pl.ds(start, block)
        parts = range(columns // LANES)
        gathered = jnp.concatenate(
            [send_rows[c, here, :] for c in parts]
            + [recv_rows[c, here, :] for c in parts],
            axis=1,
        )
        value = pre[here, :] + jnp.dot(
            gathered, w_in[columns:, :], preferred_element_type=jnp.float32
        )
        active = silu(value).astype(jnp.bfloat16)
        output = jnp.dot(active, w_out[...], preferred_element_type=jnp.float32) + b_out_ref[...]
        update = normalize(output, gain_ref[...], shift_ref[...])
        position = start + lax.broadcasted_iota(jnp.int32, (block, 1), 0)
        message = jnp.where(position < count_ref[0], update, 0.0)
        sent[here, :] = message.astype(jnp.bfloat16)
        edges[here, :] = (edges[here, :].astype(jnp.float32) + message).astype(jnp.bfloat16)
        return carry

    lax.fori_loop(0, edge_rows // block, edge_block, 0, unroll=True)

    share_rows = node_rows // shards
    pre_node = pre.at[pl.ds(0, share_rows), :]
    new = send_rows.at[:, pl.ds(0, share_rows), :]
    half = share_rows // 2
    size = half // PIECES

    def sum_at(j):
        node = j * share_rows + lax.broadcasted_iota(jnp.int32, (share_rows, LANES), 0)
        hot = [
            jnp.where(node == jnp.broadcast_to(receivers_ref[k : k + 1, :], node.shape), 1.0, 0.0)
            for k in range(edge_lines)
        ]
        sums[j] = jnp.dot(
            jnp.concatenate([v.astype(jnp.bfloat16) for v in hot], axis=1),
            sent[...],
            preferred_element_type=jnp.float32,
        ).astype(jnp.bfloat16)

    def piece_rows(k):
        return pl.ds(k * size, size)

    def piece_copy(source, target, slot, g):
        return copy_to(source, target, slot, p, g)

    sum_at(far)
    ring = []
    for k in range(PIECES):
        ring.append(piece_copy(sums.at[far, piece_rows(k), :], passed.at[0, piece_rows(k), :], PASS_RIGHT + k, right))
        ring.append(piece_copy(sums.at[far, piece_rows(PIECES + k), :], passed.at[1, piece_rows(k), :], PASS_LEFT + k, left))
    for c in ring:
        c.start()
    sum_at(right)
    plain_right = [
        piece_copy(sums.at[right, piece_rows(PIECES + k), :], plain.at[0, piece_rows(k), :], PLAIN_RIGHT + k, right)
        for k in range(PIECES)
    ]
    for c in plain_right:
        c.start()
    sum_at(left)
    plain_left = [
        piece_copy(sums.at[left, piece_rows(k), :], plain.at[1, piece_rows(k), :], PLAIN_LEFT + k, left)
        for k in range(PIECES)
    ]
    for c in plain_left:
        c.start()

    sum_copies = []
    for k in range(PIECES):
        here = piece_rows(k)
        other = piece_rows(PIECES + k)
        piece_copy(passed.at[0, here, :], passed.at[0, here, :], PASS_RIGHT + k, right).wait_recv()
        sums[right, k * size : (k + 1) * size, :] = (
            sums[right, k * size : (k + 1) * size, :].astype(jnp.float32)
            + passed[0, k * size : (k + 1) * size, :].astype(jnp.float32)
        ).astype(jnp.bfloat16)
        c = piece_copy(sums.at[right, here, :], summed.at[0, here, :], SUM_RIGHT + k, right)
        c.start()
        sum_copies.append(c)
        piece_copy(passed.at[1, here, :], passed.at[1, here, :], PASS_LEFT + k, left).wait_recv()
        sums[left, half + k * size : half + (k + 1) * size, :] = (
            sums[left, half + k * size : half + (k + 1) * size, :].astype(jnp.float32)
            + passed[1, k * size : (k + 1) * size, :].astype(jnp.float32)
        ).astype(jnp.bfloat16)
        c = piece_copy(sums.at[left, other, :], summed.at[1, here, :], SUM_LEFT + k, left)
        c.start()
        sum_copies.append(c)

    sum_at(h)
    w_node_in_in.wait()
    w_node_out_in.wait()

    def own_rows(first, count):
        there = pl.ds(pl.multiple_of(h * share_rows + first, count), count)
        return jnp.concatenate([table[c, there, :] for c in range(columns // LANES)], axis=1)

    pre_node[...] = (
        jnp.dot(
            own_rows(0, share_rows), w_node_in[:columns, :], preferred_element_type=jnp.float32
        )
        + b_node_in_ref[...]
    )

    new_copies = []
    home = []
    for k in range(PIECES):
        here = piece_rows(k)
        spans = ((k * size, 0), (half + k * size, 1))
        piece_copy(summed.at[0, here, :], summed.at[0, here, :], SUM_RIGHT + k, right).wait_recv()
        piece_copy(summed.at[1, here, :], summed.at[1, here, :], SUM_LEFT + k, left).wait_recv()
        piece_copy(plain.at[0, here, :], plain.at[0, here, :], PLAIN_RIGHT + k, right).wait_recv()
        piece_copy(plain.at[1, here, :], plain.at[1, here, :], PLAIN_LEFT + k, left).wait_recv()
        gathered = jnp.concatenate(
            [
                (
                    sums[h, first : first + size, :].astype(jnp.float32)
                    + summed[side, k * size : (k + 1) * size, :].astype(jnp.float32)
                    + plain[1 - side, k * size : (k + 1) * size, :].astype(jnp.float32)
                ).astype(jnp.bfloat16)
                for first, side in spans
            ],
            axis=0,
        )
        value = jnp.concatenate([pre_node[first : first + size, :] for first, side in spans], axis=0)
        value = value + jnp.dot(
            gathered, w_node_in[columns:, :], preferred_element_type=jnp.float32
        )
        active = silu(value).astype(jnp.bfloat16)
        output = jnp.dot(active, w_node_out[...], preferred_element_type=jnp.float32) + b_node_out_ref[...]
        update = normalize(output, node_gain_ref[...], node_shift_ref[...])
        old = jnp.concatenate([own_rows(first, size) for first, side in spans], axis=0)
        result = (old.astype(jnp.float32) + update).astype(jnp.bfloat16)
        for c in range(columns // LANES):
            for n, (first, side) in enumerate(spans):
                new[c, first : first + size, :] = result[
                    n * size : (n + 1) * size, c * LANES : (c + 1) * LANES
                ]
        for n, (first, side) in enumerate(spans):
            there = pl.ds(pl.multiple_of(h * share_rows + first, size), size)
            for m, g in enumerate((far, right, left)):
                c = piece_copy(
                    new.at[g, pl.ds(first, size), :],
                    nodes_out_ref.at[there, :],
                    NEW + (k * 2 + n) * 3 + m,
                    g,
                )
                c.start()
                new_copies.append(c)
    share_there = pl.ds(pl.multiple_of(h * share_rows, share_rows), share_rows)
    nodes_out_ref[share_there, :] = new[h]

    for c in to_right + to_left + relay_right + relay_left + pick_copies:
        c.wait_send()
    for c in halos[0] + halos[1] + halos[2]:
        c.wait_send()
    all_coarse.wait_send()
    to_twin.wait_send()
    for c in ring + plain_right + plain_left + sum_copies + new_copies:
        c.wait_send()
    for k in range(PIECES):
        for n, first in enumerate((k * size, half + k * size)):
            for m, g in enumerate((far, left, right)):
                there = pl.ds(pl.multiple_of(g * share_rows + first, size), size)
                landed = nodes_out_ref.at[there, :]
                piece_copy(landed, landed, NEW + (k * 2 + n) * 3 + m, right).wait_recv()


def layer_stage(
    nodes,
    edges,
    senders,
    receivers,
    halo_rows,
    coarse_rows,
    edge_count,
    w_edge_in,
    b_edge_in,
    w_edge_out,
    b_edge_out,
    edge_gain,
    edge_shift,
    w_node_in,
    b_node_in,
    w_node_out,
    b_node_out,
    node_gain,
    node_shift,
):
    edge_rows, columns = edges.shape
    node_rows = nodes.shape[0]
    border = halo_rows.shape[2]
    picked = coarse_rows.shape[1] * coarse_rows.shape[2]
    total = node_rows + 2 * border + picked
    shards = lax.axis_size("hidden")
    patches = lax.axis_size("patch")
    share_rows = node_rows // shards
    rounds = sum(grid_of(patches)) - 4
    vmem = pl.BlockSpec(memory_space=pltpu.VMEM)
    smem = pl.BlockSpec(memory_space=pltpu.SMEM)
    far_away = pl.BlockSpec(memory_space=pl.ANY)
    bf16 = jnp.bfloat16
    parts = columns // LANES
    network = [far_away, vmem, far_away, vmem, vmem, vmem]

    def row(v):
        return v.reshape(1, -1)

    return pl.pallas_call(
        lambda *refs: layer_kernel(COARSE_DEV, *refs),
        out_shape=(
            pltpu.VMEM(nodes.shape, bf16),
            pltpu.VMEM((edge_rows, columns), bf16),
        ),
        in_specs=[smem, far_away, far_away, vmem, vmem, vmem, vmem, *network, *network],
        out_specs=(vmem, vmem),
        scratch_shapes=[
            pltpu.VMEM((parts, total, LANES), bf16),
            pltpu.VMEM((parts, 2 * border, LANES), bf16),
            pltpu.VMEM((patches * COARSE_DEV, LANES), bf16),
            pltpu.VMEM((picked, patches * COARSE_DEV), bf16),
            pltpu.VMEM((parts, edge_rows, LANES), bf16),
            pltpu.VMEM((parts, edge_rows, LANES), bf16),
            pltpu.VMEM((edge_rows, columns), jnp.float32),
            pltpu.VMEM((edge_rows, columns), bf16),
            pltpu.VMEM(w_edge_in.shape, bf16),
            pltpu.VMEM(w_edge_out.shape, bf16),
            pltpu.VMEM(w_node_in.shape, bf16),
            pltpu.VMEM(w_node_out.shape, bf16),
            pltpu.VMEM((shards, share_rows, columns), bf16),
            pltpu.VMEM((2, share_rows // 2, columns), bf16),
            pltpu.VMEM((2, share_rows // 2, columns), bf16),
            pltpu.VMEM((2, share_rows // 2, columns), bf16),
            pltpu.SemaphoreType.DMA((SLOTS,)),
            pltpu.SemaphoreType.DMA((SLOTS,)),
            pltpu.SemaphoreType.DMA((LOCALS,)),
            pltpu.SemaphoreType.REGULAR((rounds,)),
        ],
        compiler_params=pltpu.CompilerParams(
            vmem_limit_bytes=64000000, collective_id=0, has_side_effects=True
        ),
    )(
        edge_count,
        nodes,
        edges,
        senders.reshape(-1, LANES),
        receivers.reshape(-1, LANES),
        halo_rows,
        jnp.swapaxes(coarse_rows, 1, 2),
        w_edge_in,
        row(b_edge_in),
        w_edge_out,
        row(b_edge_out),
        row(edge_gain),
        row(edge_shift),
        w_node_in,
        row(b_node_in),
        w_node_out,
        row(b_node_out),
        row(node_gain),
        row(node_shift),
    )


def solution(mesh):
    return jax.shard_map(
        layer_stage,
        mesh=mesh,
        in_specs=(
            P("patch", "hidden"),
            P(("patch", "hidden"), None),
            P(("patch", "hidden")),
            P(("patch", "hidden")),
            P("patch", None, None),
            P("patch", None, None),
            P(("patch", "hidden")),
            *([P()] * 12),
        ),
        out_specs=(P("patch", "hidden"), P(("patch", "hidden"), None)),
        check_vma=False,
    )
```
